16 devices in a mesh: dp: 2 (over y, z), tp: 8 (over x, core).
Axes of the slice: x: 4, y: 2, z: 1, core: 2. Of those that a mesh axis runs over, the one named last changes fastest.
The devices are a block of a 4x4x8 slice.
Arguments:
- hidden: bfloat16 [32, 384, 3072], P('dp', 'tp'), parts along dimension 0
- positions: int32 [32, 384], P('dp', 'tp'), parts along dimension 0
- doc_ids: int32 [32, 384], P('dp', 'tp'), parts along dimension 0
- norm_gain: bfloat16 [3072], replicated
- w_query: bfloat16 [3072, 3072], P(None, 'tp')
- w_key: bfloat16 [3072, 1024], P(None, 'tp')
- w_value: bfloat16 [3072, 1024], P(None, 'tp')
- w_out: bfloat16 [3072, 3072], P('tp')
- grad_out: bfloat16 [32, 384, 3072], P('dp', 'tp'), parts along dimension 0
Outputs:
- output 1: bfloat16 [32, 384, 3072], P('dp', 'tp'), parts along dimension 0
- output 2: bfloat16 [32, 384, 3072], P('dp', 'tp'), parts along dimension 0
- output 3: float32 [6144], P('dp'), parts along dimension 0
- output 4: float32 [6144, 3072], P('dp', 'tp'), parts along dimension 0
- output 5: float32 [6144, 1024], P('dp', 'tp'), parts along dimension 0
- output 6: float32 [6144, 1024], P('dp', 'tp'), parts along dimension 0
- output 7: float32 [6144, 3072], P(('dp', 'tp')), parts along dimension 0
There are 2 independent parts. The reference program is written for one: setup_inputs(seed, part) draws one part's arguments, and reference() takes and returns one part's arrays. A program takes and returns all parts, laid end to end along the dimension named above; an argument that names none is the same for every part.
All inputs are finite; a program needn't handle non-finite values.
Results may differ from the reference program's by a relative error of at most 0.00998037.
Values are sent between devices in bfloat16 or wider.
A program may use at most 768 MiB of HBM per device.

```python
import jax
import jax.numpy as jnp
from jax import lax

BATCH_ROWS = 16
SEQ_LEN = 384
MODEL_DIM = 3072
NUM_HEADS = 24
NUM_KV_HEADS = 8
HEAD_DIM = 128
NORM_EPS = 1e-5
ROPE_BASE = 10000.0


def draw_documents(doc_key):
    doc_mean = max(4, SEQ_LEN // 8)
    token_idx = jnp.arange(SEQ_LEN, dtype=jnp.int32)
    starts = jax.random.randint(doc_key, (BATCH_ROWS, SEQ_LEN), 0, doc_mean) == 0
    starts = starts | (token_idx == 0)[None, :]
    doc_ids = jnp.cumsum(starts.astype(jnp.int32), axis=1) - 1
    begins = lax.cummax(jnp.where(starts, token_idx[None, :], 0), axis=1)
    return (token_idx[None, :] - begins).astype(jnp.int32), doc_ids.astype(jnp.int32)


def setup_inputs(seed: int = 0, part: int = 0) -> dict:
    part_key = jax.random.fold_in(jax.random.key(seed), part)
    shared_key = jax.random.key(seed + 1)
    k_hidden, k_grad, k_doc = jax.random.split(part_key, 3)
    k_gain, k_query, k_key, k_value, k_out = jax.random.split(shared_key, 5)
    positions, doc_ids = draw_documents(k_doc)
    in_scale = MODEL_DIM ** -0.5
    out_scale = 2.0 * (NUM_HEADS * HEAD_DIM) ** -0.5
    q_width = NUM_HEADS * HEAD_DIM
    kv_width = NUM_KV_HEADS * HEAD_DIM
    return {
        'hidden': jax.random.normal(k_hidden, (BATCH_ROWS, SEQ_LEN, MODEL_DIM), jnp.float32).astype(jnp.bfloat16),
        'positions': positions,
        'doc_ids': doc_ids,
        'norm_gain': (1.0 + 0.3 * jax.random.normal(k_gain, (MODEL_DIM,), jnp.float32)).astype(jnp.bfloat16),
        'w_query': (in_scale * jax.random.normal(k_query, (MODEL_DIM, q_width), jnp.float32)).astype(jnp.bfloat16),
        'w_key': (in_scale * jax.random.normal(k_key, (MODEL_DIM, kv_width), jnp.float32)).astype(jnp.bfloat16),
        'w_value': (in_scale * jax.random.normal(k_value, (MODEL_DIM, kv_width), jnp.float32)).astype(jnp.bfloat16),
        'w_out': (out_scale * jax.random.normal(k_out, (q_width, MODEL_DIM), jnp.float32)).astype(jnp.bfloat16),
        'grad_out': jax.random.normal(k_grad, (BATCH_ROWS, SEQ_LEN, MODEL_DIM), jnp.float32).astype(jnp.bfloat16),
    }


def snap_bf16(values):
    return values + lax.stop_gradient(values.astype(jnp.bfloat16).astype(values.dtype) - values)


def rotate_pairs(values, cos_tab, sin_tab):
    pair_view = values.reshape(values.shape[:-1] + (HEAD_DIM // 2, 2))
    even_part = pair_view[..., 0]
    odd_part = pair_view[..., 1]
    turned = jnp.stack([even_part * cos_tab - odd_part * sin_tab, even_part * sin_tab + odd_part * cos_tab], axis=-1)
    return turned.reshape(values.shape)


def reference(hidden, positions, doc_ids, norm_gain, w_query, w_key, w_value, w_out, grad_out):
    group_size = NUM_HEADS // NUM_KV_HEADS
    attn_scale = HEAD_DIM ** -0.5
    inv_freq = ROPE_BASE ** (-jnp.arange(0, HEAD_DIM, 2, dtype=jnp.float32) / HEAD_DIM)
    angles = positions.astype(jnp.float32)[:, :, None] * inv_freq
    cos_tab = jnp.cos(angles)[:, :, None, :]
    sin_tab = jnp.sin(angles)[:, :, None, :]
    token_idx = jnp.arange(SEQ_LEN, dtype=jnp.int32)
    allowed = (doc_ids[:, :, None] == doc_ids[:, None, :]) & (token_idx[None, :] <= token_idx[:, None])[None]

    def head_group(operands):
        query_grp, key_grp, value_grp = operands
        scores = jnp.einsum('bqgd,bkd->bgqk', query_grp, key_grp) * attn_scale
        scores = jnp.where(allowed[:, None], scores, -1e30)
        attn_probs = snap_bf16(jax.nn.softmax(scores, axis=-1))
        return snap_bf16(jnp.einsum('bgqk,bkd->bqgd', attn_probs, value_grp))

    def forward(hidden_f32, gain_f32, wq_f32, wk_f32, wv_f32, wo_f32):
        mean_sq = jnp.mean(hidden_f32 * hidden_f32, axis=-1, keepdims=True)
        normed = snap_bf16(hidden_f32 * lax.rsqrt(mean_sq + NORM_EPS) * gain_f32)
        query_raw = jnp.dot(normed, wq_f32).reshape(BATCH_ROWS, SEQ_LEN, NUM_HEADS, HEAD_DIM)
        key_raw = jnp.dot(normed, wk_f32).reshape(BATCH_ROWS, SEQ_LEN, NUM_KV_HEADS, HEAD_DIM)
        query_rot = snap_bf16(rotate_pairs(query_raw, cos_tab, sin_tab))
        key_rot = snap_bf16(rotate_pairs(key_raw, cos_tab, sin_tab))
        value_rows = snap_bf16(jnp.dot(normed, wv_f32)).reshape(BATCH_ROWS, SEQ_LEN, NUM_KV_HEADS, HEAD_DIM)
        query_groups = jnp.moveaxis(query_rot.reshape(BATCH_ROWS, SEQ_LEN, NUM_KV_HEADS, group_size, HEAD_DIM), 2, 0)
        heads_out = lax.map(jax.checkpoint(head_group), (query_groups, jnp.moveaxis(key_rot, 2, 0), jnp.moveaxis(value_rows, 2, 0)))
        heads_flat = jnp.moveaxis(heads_out, 0, 2).reshape(BATCH_ROWS, SEQ_LEN, NUM_HEADS * HEAD_DIM)
        attn_sum = snap_bf16(jnp.dot(heads_flat, wo_f32))
        return snap_bf16(hidden_f32 + attn_sum)

    attn_out, pullback = jax.vjp(forward, hidden.astype(jnp.float32), norm_gain.astype(jnp.float32), w_query.astype(jnp.float32), w_key.astype(jnp.float32), w_value.astype(jnp.float32), w_out.astype(jnp.float32))
    grad_list = pullback(grad_out.astype(jnp.float32))
    return (attn_out.astype(jnp.bfloat16), grad_list[0].astype(jnp.bfloat16), grad_list[1], grad_list[2], grad_list[3], grad_list[4], grad_list[5])
```

```python
import functools

import jax
import jax.numpy as jnp
from jax import lax
from jax.experimental import pallas as pl
from jax.experimental.pallas import tpu as pltpu
from jax.sharding import PartitionSpec as P

HEAD_DIM = 128
NORM_EPS = 1e-5
ROPE_BASE = 10000.0
SCALE = HEAD_DIM ** -0.5
F32 = jnp.float32
BF16 = jnp.bfloat16
NT = (((1,), (1,)), ((), ()))
TN = (((0,), (0,)), ((), ()))


def swap_pairs(x):
    lane = lax.broadcasted_iota(jnp.int32, x.shape, 1)
    return jnp.where(lane % 2 == 0, pltpu.roll(x, HEAD_DIM - 1, 1), pltpu.roll(x, 1, 1))


def proj_kernel(x_ref, w_ref, cos_ref, sin_ref, q_ref, kv_ref):
    acc = jnp.dot(x_ref[...], w_ref[...], preferred_element_type=F32)
    cos, sin = cos_ref[...], sin_ref[...]
    q_heads = q_ref.shape[1] // HEAD_DIM
    for h in range(q_heads + 1):
        part = acc[:, h * HEAD_DIM:(h + 1) * HEAD_DIM]
        part = (part * cos + swap_pairs(part) * sin).astype(BF16)
        if h < q_heads:
            q_ref[:, h * HEAD_DIM:(h + 1) * HEAD_DIM] = part
        else:
            kv_ref[:, :HEAD_DIM] = part
    kv_ref[:, HEAD_DIM:] = acc[:, (q_heads + 1) * HEAD_DIM:].astype(BF16)


def project(x, w, cos, sin, tile):
    rows, width = x.shape
    cols = w.shape[1]
    q_cols = cols - 2 * HEAD_DIM
    return pl.pallas_call(
        proj_kernel,
        grid=(rows // tile,),
        in_specs=[pl.BlockSpec((tile, width), lambda m: (m, 0)),
                  pl.BlockSpec((width, cols), lambda m: (0, 0)),
                  pl.BlockSpec((tile, HEAD_DIM), lambda m: (m, 0)),
                  pl.BlockSpec((tile, HEAD_DIM), lambda m: (m, 0))],
        out_specs=[pl.BlockSpec((tile, q_cols), lambda m: (m, 0)),
                   pl.BlockSpec((tile, 2 * HEAD_DIM), lambda m: (m, 0))],
        out_shape=[jax.ShapeDtypeStruct((rows, q_cols), BF16), jax.ShapeDtypeStruct((rows, 2 * HEAD_DIM), BF16)],
        cost_estimate=pl.CostEstimate(flops=2 * rows * width * cols, bytes_accessed=2 * (rows * width + width * cols), transcendentals=0),
        name="project",
    )(x, w, cos, sin)


def block_probs(q, k, ok):
    s = lax.dot_general(q, k, NT, preferred_element_type=F32) * SCALE
    s = jnp.where(ok, s, -1e30)
    e = jnp.exp(s - jnp.max(s, axis=-1, keepdims=True))
    return e * (1.0 / jnp.sum(e, axis=-1, keepdims=True))


def allowed_block(qi_ref, ki_ref):
    kidx = ki_ref[...]
    return (kidx <= qi_ref[0, :, 0:1]) & (kidx >= qi_ref[0, :, 1:2])


def flat(ref):
    return ref[...].reshape(-1, ref.shape[-1])


def attn_fwd_kernel(q_ref, kv_ref, kr_ref, qi_ref, ki_ref, o_ref):
    ok = allowed_block(qi_ref, ki_ref)
    q, kv = flat(q_ref), jnp.concatenate([flat(kr_ref), flat(kv_ref)], axis=0)
    k, v = kv[:, :HEAD_DIM], kv[:, HEAD_DIM:]
    shape = o_ref.shape[:-1] + (HEAD_DIM,)
    for g in range(q.shape[1] // HEAD_DIM):
        cols = slice(g * HEAD_DIM, (g + 1) * HEAD_DIM)
        p = block_probs(q[:, cols], k, ok).astype(BF16)
        o = jnp.dot(p, v, preferred_element_type=F32).astype(BF16)
        o_ref[..., cols] = o.reshape(shape)


def attn_bwd_kernel(q_ref, kv_ref, kr_ref, do_ref, qi_ref, ki_ref, cos_ref, sin_ref, cosr_ref, sinr_ref,
                    dq_ref, dkv_ref, dkr_ref):
    ok = allowed_block(qi_ref, ki_ref)
    q, do = flat(q_ref), flat(do_ref)
    kv = jnp.concatenate([flat(kr_ref), flat(kv_ref)], axis=0)
    k, v = kv[:, :HEAD_DIM], kv[:, HEAD_DIM:]
    cos, sin = flat(cos_ref), flat(sin_ref)
    toks = q.shape[0]
    dk = jnp.zeros((kv.shape[0], HEAD_DIM), F32)
    dv = jnp.zeros((kv.shape[0], HEAD_DIM), F32)
    shape = dq_ref.shape[:-1] + (HEAD_DIM,)
    for g in range(q.shape[1] // HEAD_DIM):
        cols = slice(g * HEAD_DIM, (g + 1) * HEAD_DIM)
        qg, dog = q[:, cols], do[:, cols]
        p = block_probs(qg, k, ok)
        dp = lax.dot_general(dog, v, NT, preferred_element_type=F32)
        dv += lax.dot_general(p.astype(BF16), dog, TN, preferred_element_type=F32)
        row_dot = jnp.sum(p * dp, axis=-1, keepdims=True)
        ds = (p * (dp - row_dot) * SCALE).astype(BF16)
        dq = jnp.dot(ds, k, preferred_element_type=F32)
        dk += lax.dot_general(ds, qg, TN, preferred_element_type=F32)
        dq_ref[..., cols] = (dq * cos - swap_pairs(dq) * sin).astype(BF16).reshape(shape)
    dk_r, dk_l = dk[:toks], dk[toks:]
    dkv_ref[..., :HEAD_DIM] = (dk_l * cos - swap_pairs(dk_l) * sin).reshape(shape)
    dkv_ref[..., HEAD_DIM:] = dv[toks:].reshape(shape)
    dkr_ref[..., :HEAD_DIM] = (dk_r * flat(cosr_ref) - swap_pairs(dk_r) * flat(sinr_ref)).astype(BF16).reshape(shape)
    dkr_ref[..., HEAD_DIM:] = dv[:toks].astype(BF16).reshape(shape)


def row_block(width, pieces, span):
    return pl.BlockSpec((pieces, 1, span, width), lambda b: (0, b, 0, 0))


def attn_forward(q, kv, kvr, qinfo, kinfo):
    pieces, rows, span, width = q.shape
    toks = pieces * span
    return pl.pallas_call(
        attn_fwd_kernel,
        grid=(rows,),
        in_specs=[row_block(width, pieces, span), row_block(2 * HEAD_DIM, pieces, span), row_block(2 * HEAD_DIM, pieces, span),
                  pl.BlockSpec((1, toks, 2), lambda b: (b, 0, 0)), pl.BlockSpec((1, 2 * toks), lambda b: (0, 0))],
        out_specs=row_block(width, pieces, span),
        out_shape=jax.ShapeDtypeStruct(q.shape, BF16),
        cost_estimate=pl.CostEstimate(flops=16 * rows * toks * toks * width, bytes_accessed=8 * rows * toks * width, transcendentals=0),
        name="attn_fwd",
    )(q, kv, kvr, qinfo, kinfo)


def attn_backward(q, kv, kvr, do, qinfo, kinfo, tabs):
    pieces, rows, span, width = q.shape
    toks = pieces * span
    kv_spec = row_block(2 * HEAD_DIM, pieces, span)
    tab_spec = row_block(HEAD_DIM, pieces, span)
    return pl.pallas_call(
        attn_bwd_kernel,
        grid=(rows,),
        in_specs=[row_block(width, pieces, span), kv_spec, kv_spec, row_block(width, pieces, span),
                  pl.BlockSpec((1, toks, 2), lambda b: (b, 0, 0)), pl.BlockSpec((1, 2 * toks), lambda b: (0, 0)),
                  tab_spec, tab_spec, tab_spec, tab_spec],
        out_specs=[row_block(width, pieces, span), kv_spec, kv_spec],
        out_shape=[jax.ShapeDtypeStruct(q.shape, BF16), jax.ShapeDtypeStruct(kv.shape, F32), jax.ShapeDtypeStruct(kv.shape, BF16)],
        cost_estimate=pl.CostEstimate(flops=32 * rows * toks * toks * width, bytes_accessed=20 * rows * toks * width, transcendentals=0),
        name="attn_bwd",
    )(q, kv, kvr, do, qinfo, kinfo, *tabs)


def solution(mesh):
    tp = mesh.shape['tp']
    chips = tp // 2
    mates = [None] + [[(i, i ^ r) for i in range(tp)] for r in (1, 2, 3)]
    mirror = [2 * (chips - 1 - i // 2) + i % 2 for i in range(tp)]
    pair = list(enumerate(mirror))
    later = [(i, j) for i, j in pair if i < j]
    earlier = [(i, j) for i, j in pair if i > j]

    def send(x, perm, name):
        with jax.named_scope(name):
            return lax.ppermute(x, 'tp', perm)

    def device_step(hidden, positions, doc_ids, norm_gain, w_query, w_key, w_value, w_out, grad_out):
        me = lax.axis_index('tp')
        core = me % 2
        all_rows, span, width = hidden.shape
        rows = all_rows // 2
        toks = 4 * span
        split = lambda x: (lax.dynamic_slice_in_dim(x, core * rows, rows), lax.dynamic_slice_in_dim(x, (1 - core) * rows, rows))

        def join(mine, other):
            out = jnp.zeros((all_rows,) + mine.shape[1:], mine.dtype)
            out = lax.dynamic_update_slice_in_dim(out, mine, core * rows, 0)
            return lax.dynamic_update_slice_in_dim(out, other, (1 - core) * rows, 0)

        def gather(mine, other, name):
            x2 = send(mine, mates[2], name + '2')
            x3 = send(other, mates[3], name + '3')
            x1 = send(other, mates[1], name + '1')
            return jnp.stack([mine, x1, x2, x3])

        pos_loc = gather(*split(positions), 'pos')
        pos_rem = send(pos_loc, pair, 'posr')
        idx_of = lambda dev: (jnp.stack([dev ^ p for p in range(4)])[:, None] * span + jnp.arange(span)).astype(jnp.int32)
        mirror_me = 2 * (chips - 1 - me // 2) + core
        q_idx, r_idx = idx_of(me), idx_of(mirror_me)
        q_full = jnp.broadcast_to(q_idx[:, None, :], pos_loc.shape)
        qinfo = jnp.stack([q_full, q_full - pos_loc], axis=-1)
        qinfo = jnp.moveaxis(qinfo, 1, 0).reshape(rows, toks, 2)
        kinfo = jnp.concatenate([r_idx.reshape(1, toks), q_idx.reshape(1, toks)], axis=1)
        inv_freq = ROPE_BASE ** (-jnp.arange(0, HEAD_DIM, 2, dtype=F32) / HEAD_DIM)
        lane_freq = jnp.repeat(inv_freq, 2)
        lane_sign = jnp.where(jnp.arange(HEAD_DIM) % 2 == 0, -1.0, 1.0).astype(F32)

        def tables(pos):
            ang = pos.astype(F32)[..., None] * lane_freq
            return jnp.cos(ang), jnp.sin(ang) * lane_sign

        cos_l, sin_l = tables(pos_loc)
        cos_r, sin_r = tables(pos_rem)

        w_pack = jnp.concatenate([w_query, w_key, w_value], axis=1)
        wp2 = send(w_pack, pair, 'wp2')
        wo2 = send(w_out, pair, 'wo2')
        wp1 = send(w_pack, mates[1], 'wp1')
        wo1 = send(w_out, mates[1], 'wo1')
        wp3 = send(wp2, mates[1], 'wp3')
        wo3 = send(wo2, mates[1], 'wo3')
        packs = [w_pack, wp1, wp2, wp3]
        w_all = jnp.concatenate(packs, axis=1)
        wo_all = jnp.concatenate([w_out, wo1, wo2, wo3], axis=0)

        gain = norm_gain.astype(F32)

        def norm(x):
            xf = x.astype(F32)
            inv = lax.rsqrt(jnp.mean(xf * xf, axis=-1, keepdims=True) + NORM_EPS)
            return (xf * inv * gain).astype(BF16), inv

        hid_mine, hid_other = split(hidden)
        n_mine, inv_mine = norm(hid_mine)
        n_other, inv_other = norm(hid_other)
        normed = gather(n_mine, n_other, 'nrm').reshape(4 * rows * span, width)
        g_mine, g_other = split(grad_out)
        grads = gather(g_mine, g_other, 'grd').reshape(4 * rows * span, width)

        cos2, sin2 = cos_l.reshape(-1, HEAD_DIM), sin_l.reshape(-1, HEAD_DIM)
        qs, kvs, kv_in = [], [], [None] * 4
        four = lambda x: x.reshape(4, rows, span, x.shape[-1])
        for r in range(4):
            q, kv = project(normed, packs[r], cos2, sin2, rows * span)
            qs.append(four(q))
            kvs.append(four(kv))
            kv_in[r ^ 2] = send(kvs[r], later, f'kv{r}')
        heads = [None] * 4
        for r in (2, 3, 0, 1):
            heads[r] = attn_forward(qs[r], kvs[r], kv_in[r], qinfo, kinfo)
        heads_all = jnp.concatenate(heads, axis=-1).reshape(4, rows * span, -1)

        def scatter(piece_of, name):
            back = [None] * 4
            for p in (2, 3, 1):
                back[p] = send(piece_of(p).astype(BF16), mates[p], f'{name}{p}')
            mine = piece_of(0) + back[2].astype(F32)
            other = back[1].astype(F32) + back[3].astype(F32)
            return mine.reshape(rows, span, width), other.reshape(rows, span, width)

        out_piece = lambda p: jnp.dot(heads_all[p], wo_all, preferred_element_type=F32)
        a_mine, a_other = scatter(out_piece, 'att')
        attn_out = join(hid_mine + a_mine.astype(BF16), hid_other + a_other.astype(BF16))

        heads_flat = heads_all.reshape(4 * rows * span, -1)
        grad_heads = lax.dot_general(grads, wo_all, NT, preferred_element_type=F32).astype(BF16)
        do_all = four(grad_heads)
        q_cols = w_query.shape[1]

        def reduce_weights(part_of, name):
            s1 = send(part_of(1).astype(BF16), mates[1], name + '1')
            s3 = send(part_of(3).astype(BF16), mates[1], name + '3')
            s2 = send((part_of(2) + s3.astype(F32)).astype(BF16), pair, name + '2')
            return part_of(0) + s1.astype(F32) + s2.astype(F32)

        dwo = reduce_weights(lambda r: lax.dot_general(heads_flat[:, r * q_cols:(r + 1) * q_cols], grads, TN, preferred_element_type=F32), 'dwo')

        tabs = (cos_l, sin_l, cos_r, sin_r)
        dqs, dkvs, dkv_in = [None] * 4, [None] * 4, [None] * 4
        for r in range(4):
            do = do_all[..., r * q_cols:(r + 1) * q_cols]
            dqs[r], dkvs[r], dkr = attn_backward(qs[r], kvs[r], kv_in[r], do, qinfo, kinfo, tabs)
            dkv_in[r ^ 2] = send(dkr, earlier, f'dkv{r}')
        dpacks = []
        for r in range(4):
            dkv = (dkvs[r] + dkv_in[r].astype(F32)).astype(BF16)
            dpacks.append(jnp.concatenate([dqs[r], dkv], axis=-1).reshape(4 * rows * span, -1))
        d_all = jnp.concatenate(dpacks, axis=-1).reshape(4, rows * span, -1)
        in_piece = lambda p: lax.dot_general(d_all[p], w_all, NT, preferred_element_type=F32)
        gn_mine, gn_other = scatter(in_piece, 'gn')
        dwp = reduce_weights(lambda r: lax.dot_general(normed, dpacks[r], TN, preferred_element_type=F32), 'dwp')

        def norm_back(x, inv, gn, g):
            xf = x.astype(F32)
            gg = gn * gain
            part = jnp.sum(gn * xf * inv, axis=(0, 1))
            mean_term = jnp.mean(gg * xf, axis=-1, keepdims=True)
            gh = inv * gg - xf * (inv * inv * inv) * mean_term
            return (g.astype(F32) + gh).astype(BF16), part

        gh_mine, part_a = norm_back(hid_mine, inv_mine, gn_mine, g_mine)
        gh_other, part_b = norm_back(hid_other, inv_other, gn_other, g_other)
        grad_hidden = join(gh_mine, gh_other)
        gain_sum = (part_a + part_b).reshape(-1, HEAD_DIM)
        for perm, name in ((mates[1], 'gg1'), (mates[2], 'gg2'), (pair, 'gg3')):
            gain_sum = gain_sum + send(gain_sum, perm, name)
        kv_cols = w_key.shape[1]
        return (attn_out, grad_hidden, gain_sum.reshape(-1), dwp[:, :q_cols], dwp[:, q_cols:q_cols + kv_cols],
                dwp[:, q_cols + kv_cols:], dwo)

    row_spec = P('dp', 'tp', None)
    tok_spec = P('dp', 'tp')
    col_spec = P(None, 'tp')
    return jax.shard_map(
        device_step, mesh=mesh,
        in_specs=(row_spec, tok_spec, tok_spec, P(), col_spec, col_spec, col_spec, P('tp', None), row_spec),
        out_specs=(row_spec, row_spec, P('dp'), P('dp', 'tp'), P('dp', 'tp'), P('dp', 'tp'), P(('dp', 'tp'), None)),
        check_vma=False)
```

```python
import functools

import jax
import jax.numpy as jnp
from jax import lax
from jax.experimental import pallas as pl
from jax.experimental.pallas import tpu as pltpu
from jax.sharding import PartitionSpec as P


HEAD_DIM = 128
NORM_EPS = 1e-5
ROPE_BASE = 10000.0
SCALE = HEAD_DIM ** -0.5
LOG2E = 1.4426950408889634
F32 = jnp.float32
BF16 = jnp.bfloat16
NN = (((1,), (0,)), ((), ()))
NT = (((1,), (1,)), ((), ()))
TN = (((0,), (0,)), ((), ()))
VMEM_LIMIT = 63000 * 1024
GROUPS = (1, 3, 0, 2)
SLOT = {g: s for s, g in enumerate(GROUPS)}
ANY = pl.BlockSpec(memory_space=pl.ANY)


def dot(a, b, dims):
    return lax.dot_general(a, b, dims, preferred_element_type=F32)


def cost(flops, size):
    return pl.CostEstimate(flops=int(flops), bytes_accessed=int(size), transcendentals=0)


def swap_pairs(x):
    lane = lax.broadcasted_iota(jnp.int32, x.shape, 1)
    return jnp.where(lane % 2 == 0, pltpu.roll(x, HEAD_DIM - 1, 1), pltpu.roll(x, 1, 1))


def place_kernel(normalize, x_ref, gain_ref, *refs):
    x = x_ref[...]
    if normalize:
        xf = x.astype(F32)
        inv = lax.rsqrt(jnp.mean(xf * xf, axis=-1, keepdims=True) + NORM_EPS)
        x = (xf * inv * gain_ref[...]).astype(BF16)
    refs[-1][...] = x


def place(x, gain, buf, at, axis, normalize=False):
    rows, width = x.shape
    steps = 4
    tile = rows // steps
    shape = (4 * rows, width) if axis == 0 else (rows, 4 * width)
    where = (lambda m: (at * steps + m, 0)) if axis == 0 else (lambda m: (m, at))
    ops, specs, alias = (x, gain), [pl.BlockSpec((tile, width), lambda m: (m, 0)), pl.BlockSpec(gain.shape, lambda m: (0, 0))], {}
    if buf is not None:
        ops, specs, alias = ops + (buf,), specs + [ANY], {2: 0}
    return pl.pallas_call(
        functools.partial(place_kernel, normalize), grid=(steps,), in_specs=specs, out_specs=pl.BlockSpec((tile, width), where),
        out_shape=jax.ShapeDtypeStruct(shape, BF16), input_output_aliases=alias,
        cost_estimate=cost(1000 * rows * width, 4 * rows * width), name="place")(*ops)


def proj_kernel(turned, x_ref, w_ref, cos_ref, sin_ref, o_ref):
    chunk = x_ref.shape[0] // 4
    for m in range(4):
        rows = slice(m * chunk, (m + 1) * chunk)
        acc = dot(x_ref[rows], w_ref[...], NN)
        for h in range(acc.shape[1] // HEAD_DIM):
            cols = slice(h * HEAD_DIM, (h + 1) * HEAD_DIM)
            part = acc[:, cols]
            if h < turned:
                part = part * cos_ref[rows] + swap_pairs(part) * sin_ref[rows]
            o_ref[rows, cols] = part.astype(BF16)


def project(x, w, cos, sin, first, count, turned):
    rows, width = x.shape
    tile = 2 * HEAD_DIM
    whole = lambda a: pl.BlockSpec(a.shape, lambda n: (0, 0))
    return pl.pallas_call(
        functools.partial(proj_kernel, turned), grid=(count,),
        in_specs=[whole(x), pl.BlockSpec((width, tile), lambda n: (0, first + n)), whole(cos), whole(sin)],
        out_specs=pl.BlockSpec((rows, tile), lambda n: (0, n)),
        out_shape=jax.ShapeDtypeStruct((rows, count * tile), BF16),
        compiler_params=pltpu.CompilerParams(vmem_limit_bytes=VMEM_LIMIT),
        cost_estimate=cost(2 * rows * width * count * tile, 2 * rows * width), name="project")(x, w, cos, sin)


def token_rows(ref, b):
    x = ref[:, b] if len(ref.shape) == 4 else ref[b]
    return x.reshape(-1, x.shape[-1])


def by_head(x):
    return jnp.concatenate([x[:, h * HEAD_DIM:(h + 1) * HEAD_DIM] for h in range(x.shape[1] // HEAD_DIM)], axis=0)


def allowed_block(qi_ref, ki_ref, b):
    kidx = ki_ref[...]
    return (kidx <= qi_ref[b, :, 0:1]) & (kidx >= qi_ref[b, :, 1:2])


def probs(q, k, ok):
    s = dot(q, k, NT).reshape(-1, ok.shape[0], ok.shape[1])
    s = jnp.where(ok[None], s, -1e30)
    e = jnp.exp2((s - jnp.max(s, axis=-1, keepdims=True)) * (SCALE * LOG2E))
    return e * (1.0 / jnp.sum(e, axis=-1, keepdims=True))


def keys_values(kr_ref, kv_ref, b):
    kv = jnp.concatenate([token_rows(kr_ref, b), token_rows(kv_ref, b)], axis=0)
    return kv[:, :HEAD_DIM], kv[:, HEAD_DIM:]


def attn_fwd_kernel(q_ref, kv_ref, kr_ref, qi_ref, ki_ref, *refs):
    o_ref = refs[-1]
    shape = (o_ref.shape[0], o_ref.shape[2], HEAD_DIM)
    for b in range(q_ref.shape[1]):
        ok = allowed_block(qi_ref, ki_ref, b)
        k, v = keys_values(kr_ref, kv_ref, b)
        p = probs(by_head(token_rows(q_ref, b)), k, ok).astype(BF16).reshape(-1, k.shape[0])
        o = dot(p, v, NN).astype(BF16)
        toks = ok.shape[0]
        for h in range(o.shape[0] // toks):
            o_ref[:, b, :, h * HEAD_DIM:(h + 1) * HEAD_DIM] = o[h * toks:(h + 1) * toks].reshape(shape)


def attn_bwd_kernel(n_alias, q_ref, kv_ref, kr_ref, do0_ref, do1_ref, do2_ref, do3_ref, qi_ref, ki_ref, cos_ref, sin_ref, cosr_ref, sinr_ref, *refs):
    dq_ref, dkv_ref, dkr_ref = refs[n_alias:]
    shape = (dq_ref.shape[0], dq_ref.shape[2], HEAD_DIM)
    for b in range(q_ref.shape[1]):
        ok = allowed_block(qi_ref, ki_ref, b)
        toks = ok.shape[0]
        q = by_head(token_rows(q_ref, b))
        do = by_head(jnp.concatenate([token_rows(d, b) for d in (do0_ref, do1_ref, do2_ref, do3_ref)], axis=0))
        k, v = keys_values(kr_ref, kv_ref, b)
        p = probs(q, k, ok)
        dp = dot(do, v, NT).reshape(p.shape)
        p_low = p.astype(BF16).reshape(-1, k.shape[0])
        dv = dot(p_low, do, TN)
        ds = (p * (dp - jnp.sum(p * dp, axis=-1, keepdims=True))).astype(BF16).reshape(p_low.shape)
        dq = dot(ds, k, NN) * SCALE
        dk = dot(ds, q, TN) * SCALE
        cos, sin = token_rows(cos_ref, b), token_rows(sin_ref, b)
        for h in range(dq.shape[0] // toks):
            part = dq[h * toks:(h + 1) * toks]
            dq_ref[:, b, :, h * HEAD_DIM:(h + 1) * HEAD_DIM] = (part * cos - swap_pairs(part) * sin).astype(BF16).reshape(shape)
        dk_r, dk_l = dk[:toks], dk[toks:]
        dkv_ref[:, b, :, :HEAD_DIM] = (dk_l * cos - swap_pairs(dk_l) * sin).reshape(shape)
        dkv_ref[:, b, :, HEAD_DIM:] = dv[toks:].reshape(shape)
        dkr_ref[:, b, :, :HEAD_DIM] = (dk_r * token_rows(cosr_ref, b) - swap_pairs(dk_r) * token_rows(sinr_ref, b)).astype(BF16).reshape(shape)
        dkr_ref[:, b, :, HEAD_DIM:] = dv[:toks].astype(BF16).reshape(shape)


ROWS_PER_STEP = 2


def block_at(pieces, span, width, col):
    return pl.BlockSpec((pieces, ROWS_PER_STEP, span, width), lambda b: (0, b, 0, col))


def attn_specs(group, q_cols, pieces, span):
    toks = pieces * span
    s, t = SLOT[group], SLOT[group ^ 2]
    kv_cols = 2 * HEAD_DIM
    return ([block_at(pieces, span, q_cols, s), block_at(pieces, span, kv_cols, s % 2), block_at(pieces, span, kv_cols, t % 2)],
            [pl.BlockSpec((ROWS_PER_STEP, toks, 2), lambda b: (b, 0, 0)), pl.BlockSpec((1, 2 * toks), lambda b: (0, 0))])


def attn_forward(group, q, kv, kvr, qinfo, kinfo, buf):
    pieces, rows, span, q_all = q.shape
    q_cols, toks = q_all // 4, pieces * span
    big, info = attn_specs(group, q_cols, pieces, span)
    ops, specs, alias = (q, kv, kvr, qinfo, kinfo), big + info, {}
    if buf is not None:
        ops, specs, alias = ops + (buf,), specs + [ANY], {5: 0}
    return pl.pallas_call(
        attn_fwd_kernel, grid=(rows // ROWS_PER_STEP,), in_specs=specs, out_specs=block_at(pieces, span, q_cols, SLOT[group]),
        out_shape=jax.ShapeDtypeStruct(q.shape, BF16), input_output_aliases=alias,
        compiler_params=pltpu.CompilerParams(vmem_limit_bytes=VMEM_LIMIT),
        cost_estimate=cost(8 * rows * toks * toks * q_cols, 8 * rows * toks * q_cols), name="attn_fwd")(*ops)


def attn_backward(group, q, kv, kvr, dos, qinfo, kinfo, tabs, bufs):
    pieces, rows, span, q_all = q.shape
    q_cols, toks, s = q_all // 4, pieces * span, SLOT[group]
    kv_cols = 2 * HEAD_DIM
    big, info = attn_specs(group, q_cols, pieces, span)
    do_spec = pl.BlockSpec((ROWS_PER_STEP, span, q_cols), lambda b: (b, 0, s))
    ops = (q, kv, kvr, *dos, qinfo, kinfo, *tabs)
    specs, alias = big + [do_spec] * 4 + info + [block_at(pieces, span, HEAD_DIM, 0)] * 4, {}
    n_alias = 0
    for i, buf in enumerate(bufs):
        if buf is not None:
            alias[len(ops)] = i
            ops, specs, n_alias = ops + (buf,), specs + [ANY], n_alias + 1
    half = (pieces, rows, span, 2 * kv_cols)
    return pl.pallas_call(
        functools.partial(attn_bwd_kernel, n_alias), grid=(rows // ROWS_PER_STEP,), in_specs=specs,
        out_specs=[block_at(pieces, span, q_cols, s), block_at(pieces, span, kv_cols, s % 2), block_at(pieces, span, kv_cols, s % 2)],
        out_shape=[jax.ShapeDtypeStruct(q.shape, BF16), jax.ShapeDtypeStruct(half, F32), jax.ShapeDtypeStruct(half, BF16)],
        input_output_aliases=alias, compiler_params=pltpu.CompilerParams(vmem_limit_bytes=VMEM_LIMIT),
        cost_estimate=cost(20 * rows * toks * toks * q_cols, 20 * rows * toks * q_cols), name="attn_bwd")(*ops)


def grad_in_kernel(dq_ref, da_ref, db_ref, wq_ref, wkv_ref, first_ref, second_ref):
    half = da_ref.shape[1]
    out = dot(dq_ref[...], wq_ref[...], NT) + dot(da_ref[...], wkv_ref[:, :half], NT) + dot(db_ref[...], wkv_ref[:, half:], NT)
    rows = first_ref.shape[0]
    first_ref[...] = out[:rows].astype(first_ref.dtype)
    second_ref[...] = out[rows:].astype(second_ref.dtype)


def grad_in(dq, da, db, wq, wkv, pair_at, types):
    rows, tile = dq.shape[0] // 2, 2 * HEAD_DIM
    half = lambda a: pl.BlockSpec((rows, a.shape[1]), lambda n: (pair_at, 0))
    row = lambda a: pl.BlockSpec((tile, a.shape[1]), lambda n: (n, 0))
    out = pl.BlockSpec((rows // 2, tile), lambda n: (0, n))
    width = wq.shape[0]
    return pl.pallas_call(
        grad_in_kernel, grid=(width // tile,), in_specs=[half(dq), half(da), half(db), row(wq), row(wkv)], out_specs=[out, out],
        out_shape=[jax.ShapeDtypeStruct((rows // 2, width), t) for t in types],
        compiler_params=pltpu.CompilerParams(vmem_limit_bytes=VMEM_LIMIT),
        cost_estimate=cost(2 * rows * width * (wq.shape[1] + wkv.shape[1]), 4 * rows * width), name="grad_in")(dq, da, db, wq, wkv)


def head_out_kernel(h_ref, w_ref, first_ref, second_ref):
    out = dot(h_ref[...], w_ref[...], NN)
    rows = first_ref.shape[0]
    first_ref[...] = out[:rows].astype(first_ref.dtype)
    second_ref[...] = out[rows:].astype(second_ref.dtype)


def head_out(heads, w, pair_at, types):
    rows, inner, width, tile = heads.shape[0] // 2, heads.shape[1], w.shape[1], 4 * HEAD_DIM
    out = pl.BlockSpec((rows // 2, tile), lambda n: (0, n))
    return pl.pallas_call(
        head_out_kernel, grid=(width // tile,),
        in_specs=[pl.BlockSpec((rows, inner), lambda n: (pair_at, 0)), pl.BlockSpec((inner, tile), lambda n: (0, n))], out_specs=[out, out],
        out_shape=[jax.ShapeDtypeStruct((rows // 2, width), t) for t in types],
        compiler_params=pltpu.CompilerParams(vmem_limit_bytes=VMEM_LIMIT),
        cost_estimate=cost(2 * rows * width * inner, 4 * rows * width), name="head_out")(heads, w)


def residual_kernel(x_ref, a_ref, b_ref, *refs):
    total = a_ref[...].astype(F32) + b_ref[...].astype(F32)
    refs[-1][...] = (x_ref[...].astype(F32) + total.astype(BF16).astype(F32)).astype(BF16)


def norm_back_kernel(x_ref, g_ref, a_ref, b_ref, gain_ref, *refs):
    gh_ref, part_ref = refs[-2:]
    tile, width = x_ref.shape
    chunk = 2 * HEAD_DIM
    cuts = [slice(c, c + chunk) for c in range(0, width, chunk)]

    @pl.when(pl.program_id(0) == 0)
    def _():
        part_ref[...] = jnp.zeros_like(part_ref)

    def load(cols):
        return x_ref[:, cols].astype(F32), a_ref[:, cols].astype(F32) + b_ref[:, cols].astype(F32)

    square, cross = jnp.zeros((tile, chunk), F32), jnp.zeros((tile, chunk), F32)
    for cols in cuts:
        x, gn = load(cols)
        square += x * x
        cross += gn * gain_ref[:, cols] * x
    inv = lax.rsqrt(jnp.sum(square, axis=-1, keepdims=True) / width + NORM_EPS)
    slope = inv * inv * inv * (jnp.sum(cross, axis=-1, keepdims=True) / width)
    for cols in cuts:
        x, gn = load(cols)
        scaled = gn * inv
        gh_ref[:, cols] = (g_ref[:, cols].astype(F32) + (scaled * gain_ref[:, cols] - x * slope)).astype(BF16)
        part_ref[:, cols] += jnp.sum((scaled * x).reshape(-1, 8, chunk), axis=0)


def half_rows_call(kernel, half, arrays, gain, buf, out_shape, with_part):
    rows, width = arrays[-1].shape
    steps = 4
    tile = rows // steps
    mine = pl.BlockSpec((tile, width), lambda m, h: (m, 0))
    full = pl.BlockSpec((tile, width), lambda m, h: (h[0] * steps + m, 0))
    specs = [full if a.shape[0] == out_shape[0] else mine for a in arrays]
    ops, alias = tuple(arrays), {}
    if gain is not None:
        ops, specs = ops + (gain,), specs + [pl.BlockSpec(gain.shape, lambda m, h: (0, 0))]
    if buf is not None:
        alias = {1 + len(ops): 0}
        ops, specs = ops + (buf,), specs + [ANY]
    outs, out_specs = [jax.ShapeDtypeStruct(out_shape, BF16)], [full]
    if with_part:
        outs.append(jax.ShapeDtypeStruct((8, width), F32))
        out_specs.append(pl.BlockSpec((8, width), lambda m, h: (0, 0)))

    def body(h_ref, *refs):
        kernel(*refs)

    return pl.pallas_call(
        body, grid_spec=pltpu.PrefetchScalarGridSpec(num_scalar_prefetch=1, grid=(steps,), in_specs=specs, out_specs=out_specs),
        out_shape=outs, input_output_aliases=alias, cost_estimate=cost(1000 * rows * width, 10 * rows * width))(half, *ops)


def solution(mesh):
    tp = mesh.shape['tp']
    chips = tp // 2
    mirror = [2 * (chips - 1 - i // 2) + i % 2 for i in range(tp)]
    mates = [[(i, i ^ r) for i in range(tp)] for r in range(4)]
    far = [[(mirror[i] ^ r, i) for i in range(tp)] for r in range(4)]
    pair = list(enumerate(mirror))
    later = [(i, j) for i, j in pair if i < j]
    earlier = [(i, j) for i, j in pair if i > j]

    def send(x, perm):
        return lax.ppermute(x, 'tp', perm)

    def device_step(hidden, positions, doc_ids, norm_gain, w_query, w_key, w_value, w_out, grad_out):
        last = []

        def run(fn, *args):
            if last:
                *args, _ = lax.optimization_barrier((*args, last[0]))
            out = fn(*args)
            last[:] = [jax.tree.leaves(out)[0]]
            return out

        def after(x):
            return lax.optimization_barrier((x, last[0]))[0]

        me = lax.axis_index('tp')
        core = me % 2
        all_rows, span, width = hidden.shape
        rows = all_rows // 2
        toks = 4 * span
        q_cols = w_query.shape[1]
        split = lambda x: (lax.dynamic_slice_in_dim(x, core * rows, rows), lax.dynamic_slice_in_dim(x, (1 - core) * rows, rows))
        four = lambda x: x.reshape(4, rows, span, x.shape[-1])
        flat = lambda x: x.reshape(-1, x.shape[-1])

        hid_mine, hid_other = split(hidden)
        hid2 = send(hid_mine, mates[2])
        hid1 = send(hid_other, mates[1])
        w_kv = jnp.concatenate([w_key, w_value], axis=1)
        wkv2 = send(w_kv, pair)
        wkv1 = send(w_kv, mates[1])
        wq1 = send(w_query, mates[1])
        pos_mine, pos_other = split(positions)
        by_piece = (pos_mine, pos_other, pos_mine, pos_other)
        pos_loc = [pos_mine] + [send(by_piece[p], mates[p]) for p in (1, 2, 3)]
        pos_rem = [send(by_piece[p], far[p]) for p in range(4)]
        wq2 = send(w_query, pair)
        hid3 = send(hid_other, mates[3])
        wo1 = send(w_out, mates[1])
        wo2 = send(w_out, pair)
        g_mine, g_other = split(grad_out)
        grd1 = send(g_other, mates[1])
        grd2 = send(g_mine, mates[2])
        grd3 = send(g_other, mates[3])

        gain_row = norm_gain.astype(F32)[None]

        def put(x, buf, at, axis, normalize=False):
            if buf is None:
                return run(lambda x_: place(x_, gain_row, None, at, axis, normalize), x)
            return run(lambda x_, b: place(x_, gain_row, b, at, axis, normalize), x, buf)

        wq_all = put(w_query, None, SLOT[0], 1)
        wkv_all = put(w_kv, None, SLOT[0], 1)
        wo_all = put(w_out, None, SLOT[0], 0)
        normed = put(flat(hid_mine), None, 0, 0, True)
        grads = put(flat(g_mine), None, 0, 0)
        normed = put(flat(hid1), normed, 1, 0, True)
        wkv_all = put(wkv1, wkv_all, SLOT[1], 1)
        wq_all = put(wq1, wq_all, SLOT[1], 1)
        wo_all = put(wo1, wo_all, SLOT[1], 0)
        grads = put(flat(grd1), grads, 1, 0)
        wkv3 = send(after(wkv2), mates[1])
        wkv_all = put(wkv2, wkv_all, SLOT[2], 1)
        wkv_all = put(wkv3, wkv_all, SLOT[3], 1)
        normed = put(flat(hid2), normed, 2, 0, True)

        pos_loc, pos_rem = jnp.stack(pos_loc), jnp.stack(pos_rem)
        pos_loc, pos_rem = after((pos_loc, pos_rem))
        idx_of = lambda dev: (jnp.stack([dev ^ p for p in range(4)])[:, None] * span + jnp.arange(span)).astype(jnp.int32)
        q_idx, r_idx = idx_of(me), idx_of(2 * (chips - 1 - me // 2) + core)
        q_full = jnp.broadcast_to(q_idx[:, None, :], pos_loc.shape)
        qinfo = jnp.stack([q_full, q_full - pos_loc], axis=-1)
        qinfo = jnp.moveaxis(qinfo, 1, 0).reshape(rows, toks, 2)
        kinfo = jnp.concatenate([r_idx.reshape(1, toks), q_idx.reshape(1, toks)], axis=1)
        inv_freq = ROPE_BASE ** (-jnp.arange(0, HEAD_DIM, 2, dtype=F32) / HEAD_DIM)
        lane_freq = jnp.repeat(inv_freq, 2)
        lane_sign = jnp.where(jnp.arange(HEAD_DIM) % 2 == 0, -1.0, 1.0).astype(F32)

        def tables(pos):
            ang = pos.astype(F32)[..., None] * lane_freq
            return jnp.cos(ang), jnp.sin(ang) * lane_sign

        cos_l, sin_l = tables(pos_loc)
        cos_r, sin_r = tables(pos_rem)
        cos2, sin2 = flat(cos_l), flat(sin_l)
        cos2, sin2, qinfo, kinfo, cos_r, sin_r = lax.optimization_barrier((cos2, sin2, qinfo, kinfo, cos_r, sin_r))
        last[:] = [cos2]
        tabs = (four(cos2), four(sin2), cos_r, sin_r)

        wq3 = send(after(wq2), mates[1])
        wq_all = put(wq2, wq_all, SLOT[2], 1)
        wq_all = put(wq3, wq_all, SLOT[3], 1)
        normed = put(flat(hid3), normed, 3, 0, True)

        kvs, kv_in = [], []
        for i in range(2):
            kv = four(run(lambda x, w: project(x, w, cos2, sin2, 2 * i, 2, 1), normed, wkv_all))
            kvs.append(kv)
            kv_in.append(send(kv, later))
        q_all = four(run(lambda x, w: project(x, w, cos2, sin2, 0, 2 * q_cols // HEAD_DIM, 2), normed, wq_all))
        wo3 = send(after(wo2), mates[1])
        wo_all = put(wo2, wo_all, SLOT[2], 0)
        wo_all = put(wo3, wo_all, SLOT[3], 0)
        head_grad = lambda g, w: dot(g, w, NT).astype(BF16).reshape(rows, span, -1)
        dos = [run(head_grad, flat(g), wo_all) for g in (g_mine, grd1, grd2)]
        grads = put(flat(grd2), grads, 2, 0)
        heads = None
        for g in GROUPS:
            local, far_in = kvs[SLOT[g] // 2], kv_in[SLOT[g ^ 2] // 2]
            if heads is None:
                heads = run(lambda q, kv, kr: attn_forward(g, q, kv, kr, qinfo, kinfo, None), q_all, local, far_in)
            else:
                heads = run(lambda q, kv, kr, h: attn_forward(g, q, kv, kr, qinfo, kinfo, h), q_all, local, far_in, heads)
        heads_flat = flat(heads)
        att = [None] * 4
        out2, out3 = run(lambda h, w: head_out(h, w, 1, (BF16, BF16)), heads_flat, wo_all)
        att[2], att[3] = send(out2, mates[2]), send(out3, mates[3])
        own_out, out1 = run(lambda h, w: head_out(h, w, 0, (F32, BF16)), heads_flat, wo_all)
        att[1] = send(out1, mates[1])

        dos.append(run(head_grad, flat(grd3), wo_all))
        dq, dkv, dkr, dkv_in = None, [None, None], [None, None], [None, None]
        for g in GROUPS:
            i = SLOT[g] // 2
            bufs = [b for b in (dq, dkv[i], dkr[i]) if b is not None]
            given = tuple(b is not None for b in (dq, dkv[i], dkr[i]))

            def fn(q, kv, kr, d0, d1, d2, d3, *rest):
                it = iter(rest)
                return attn_backward(g, q, kv, kr, (d0, d1, d2, d3), qinfo, kinfo, tabs, [next(it) if ok else None for ok in given])

            dq, dkv[i], dkr[i] = run(fn, q_all, kvs[i], kv_in[SLOT[g ^ 2] // 2], *dos, *bufs)
            if SLOT[g] % 2 == 1:
                dkv_in[i] = send(dkr[i], earlier)

        def add_far(mine, theirs):
            swapped = jnp.concatenate([theirs[..., 2 * HEAD_DIM:], theirs[..., :2 * HEAD_DIM]], axis=-1)
            return flat((mine + swapped.astype(F32)).astype(BF16))

        grads = put(flat(grd3), grads, 3, 0)
        cut = lambda x, s, n: x[:, s * q_cols:(s + n) * q_cols]
        so13 = send(run(lambda h, g: dot(cut(h, 0, 2), g, TN).astype(BF16), heads_flat, grads), mates[1])
        dq_flat = flat(dq)
        low = lambda x: x.astype(BF16)
        spq13 = send(run(lambda d, n: low(dot(n, cut(d, 0, 2), TN)), dq_flat, normed), mates[1])
        dkv_a = run(add_far, dkv[0], dkv_in[0])
        spk13 = send(run(lambda d, n: low(dot(n, d, TN)), dkv_a, normed), mates[1])
        so1, so3 = run(lambda e: (e[:q_cols], e[q_cols:]), so13)
        so2 = send(run(lambda h, gg, e: (dot(cut(h, 3, 1), gg, TN) + e.astype(F32)).astype(BF16), heads_flat, grads, so3), pair)
        mine_half, other_half = core.astype(jnp.int32)[None], (1 - core).astype(jnp.int32)[None]
        flat_shape = (all_rows * span, width)
        hid_flat, g_flat = flat(hidden), flat(grad_out)
        dkv_b = run(add_far, dkv[1], dkv_in[1])
        both = run(lambda d, a, b, wq, wk: grad_in(d, a, b, wq, wk, 1, (BF16, BF16)), dq_flat, dkv_a, dkv_b, wq_all, wkv_all)
        gn2, gn3 = send(both[0], mates[2]), send(both[1], mates[3])
        spq2 = send(run(lambda d, n, e: low(dot(n, cut(d, 3, 1), TN) + e[:, q_cols:].astype(F32)), dq_flat, normed, spq13), pair)
        kv_half = 2 * HEAD_DIM
        spk2 = send(run(lambda d, n, e: low(dot(n, d[:, kv_half:], TN) + e[:, kv_half:].astype(F32)), dkv_b, normed, spk13), pair)
        own_in, gn1 = run(lambda d, a, b, wq, wk: grad_in(d, a, b, wq, wk, 0, (F32, BF16)), dq_flat, dkv_a, dkv_b, wq_all, wkv_all)
        gn1 = send(gn1, mates[1])
        attn_out = run(lambda x, a, b: half_rows_call(residual_kernel, mine_half, (x, a, b), None, None, flat_shape, False)[0], hid_flat, own_out, flat(att[2]))
        attn_out = run(lambda x, a, b, o: half_rows_call(residual_kernel, other_half, (x, a, b), None, o, flat_shape, False)[0], hid_flat, flat(att[1]), flat(att[3]), attn_out)
        back_call = lambda h, arrays, buf: half_rows_call(norm_back_kernel, h, arrays, gain_row, buf, flat_shape, True)
        grad_hidden, part_a = run(lambda x, g, a, b: back_call(mine_half, (x, g, a, b), None), hid_flat, g_flat, own_in, gn2)
        dwo = run(lambda h, g, a, b: dot(cut(h, 2, 1), g, TN) + a.astype(F32) + b.astype(F32), heads_flat, grads, so1, so2)
        own_q = after(run(lambda d, n, e: dot(n, cut(d, 2, 1), TN) + e[:, :q_cols].astype(F32), dq_flat, normed, spq13))
        own_kv = after(run(lambda d, n, e: dot(n, d[:, :kv_half], TN) + e[:, :kv_half].astype(F32), dkv_b, normed, spk13))
        grad_hidden, part_b = run(lambda x, g, a, b, o: back_call(other_half, (x, g, a, b), o), hid_flat, g_flat, gn1, gn3, grad_hidden)
        gain_sum = jnp.sum(part_a + part_b, axis=0).reshape(-1, HEAD_DIM)
        for perm in (mates[1], mates[2], pair):
            gain_sum = gain_sum + send(gain_sum, perm)
        dwq = own_q + spq2.astype(F32)
        dwk = own_kv[:, :HEAD_DIM] + spk2[:, :HEAD_DIM].astype(F32)
        dwv = own_kv[:, HEAD_DIM:] + spk2[:, HEAD_DIM:].astype(F32)
        return attn_out.reshape(hidden.shape), grad_hidden.reshape(hidden.shape), gain_sum.reshape(-1), dwq, dwk, dwv, dwo

    row_spec = P('dp', 'tp', None)
    tok_spec = P('dp', 'tp')
    col_spec = P(None, 'tp')
    return jax.shard_map(
        device_step, mesh=mesh,
        in_specs=(row_spec, tok_spec, tok_spec, P(), col_spec, col_spec, col_spec, P('tp', None), row_spec),
        out_specs=(row_spec, row_spec, P('dp'), P('dp', 'tp'), P('dp', 'tp'), P('dp', 'tp'), P(('dp', 'tp'), None)),
        check_vma=False)
```

```python
import functools

import jax
import jax.numpy as jnp
from jax import lax
from jax.experimental import pallas as pl
from jax.experimental.pallas import tpu as pltpu
from jax.sharding import PartitionSpec as P


HEAD_DIM = 128
NORM_EPS = 1e-5
ROPE_BASE = 10000.0
SCALE = HEAD_DIM ** -0.5
LOG2E = 1.4426950408889634
F32 = jnp.float32
BF16 = jnp.bfloat16
NN = (((1,), (0,)), ((), ()))
NT = (((1,), (1,)), ((), ()))
TN = (((0,), (0,)), ((), ()))
VMEM_LIMIT = 63000 * 1024
GROUPS = (1, 3, 0, 2)
SLOT = {g: s for s, g in enumerate(GROUPS)}
ANY = pl.BlockSpec(memory_space=pl.ANY)


def dot(a, b, dims):
    return lax.dot_general(a, b, dims, preferred_element_type=F32)


def cost(flops, size):
    return pl.CostEstimate(flops=int(flops), bytes_accessed=int(size), transcendentals=0)


def swap_pairs(x):
    lane = lax.broadcasted_iota(jnp.int32, x.shape, 1)
    return jnp.where(lane % 2 == 0, pltpu.roll(x, HEAD_DIM - 1, 1), pltpu.roll(x, 1, 1))


def place_kernel(normalize, x_ref, gain_ref, *refs):
    x = x_ref[...]
    if normalize:
        xf = x.astype(F32)
        inv = lax.rsqrt(jnp.mean(xf * xf, axis=-1, keepdims=True) + NORM_EPS)
        x = (xf * inv * gain_ref[...]).astype(BF16)
    refs[-1][...] = x


def place(x, gain, buf, at, axis, normalize=False):
    rows, width = x.shape
    steps = 2
    tile = rows // steps
    shape = (4 * rows, width) if axis == 0 else (rows, 4 * width)
    where = (lambda m: (at * steps + m, 0)) if axis == 0 else (lambda m: (m, at))
    ops, specs, alias = (x, gain), [pl.BlockSpec((tile, width), lambda m: (m, 0)), pl.BlockSpec(gain.shape, lambda m: (0, 0))], {}
    if buf is not None:
        ops, specs, alias = ops + (buf,), specs + [ANY], {2: 0}
    return pl.pallas_call(
        functools.partial(place_kernel, normalize), grid=(steps,), in_specs=specs, out_specs=pl.BlockSpec((tile, width), where),
        out_shape=jax.ShapeDtypeStruct(shape, BF16), input_output_aliases=alias,
        cost_estimate=cost(1000 * rows * width, 4 * rows * width), name="place")(*ops)


def proj_kernel(turned, chunk, x_ref, w_ref, cos_ref, sin_ref, *refs):
    o_ref = refs[-1]
    for m in range(0, x_ref.shape[0], chunk):
        rows = slice(m, m + chunk)
        acc = dot(x_ref[rows], w_ref[...], NN)
        for h in range(acc.shape[1] // HEAD_DIM):
            cols = slice(h * HEAD_DIM, (h + 1) * HEAD_DIM)
            part = acc[:, cols]
            if h < turned:
                part = part * cos_ref[rows] + swap_pairs(part) * sin_ref[rows]
            o_ref[rows, cols] = part.astype(BF16)


def project(x, w, cos, sin, first, count, turned, span=None, buf=None):
    rows, width = x.shape
    tile, chunk = 2 * HEAD_DIM, rows // 4
    at, part = span or (0, rows)
    some = lambda a: pl.BlockSpec((part, a.shape[1]), lambda n: (at, 0))
    ops, alias = (x, w, cos, sin), {}
    specs = [some(x), pl.BlockSpec((width, tile), lambda n: (0, first + n)), some(cos), some(sin)]
    if buf is not None:
        alias = {len(ops): 0}
        ops, specs = ops + (buf,), specs + [ANY]
    return pl.pallas_call(
        functools.partial(proj_kernel, turned, chunk), grid=(count,), in_specs=specs,
        out_specs=pl.BlockSpec((part, tile), lambda n: (at, n)), input_output_aliases=alias,
        out_shape=jax.ShapeDtypeStruct((rows, count * tile), BF16),
        compiler_params=pltpu.CompilerParams(vmem_limit_bytes=VMEM_LIMIT),
        cost_estimate=cost(2 * part * width * count * tile, 2 * part * width), name="project")(*ops)


def token_rows(ref, b):
    x = ref[:, b] if len(ref.shape) == 4 else ref[b]
    return x.reshape(-1, x.shape[-1])


def by_head(x):
    return jnp.concatenate([x[:, h * HEAD_DIM:(h + 1) * HEAD_DIM] for h in range(x.shape[1] // HEAD_DIM)], axis=0)


def allowed_block(qi_ref, ki_ref, b):
    kidx = ki_ref[...]
    return (kidx <= qi_ref[b, :, 0:1]) & (kidx >= qi_ref[b, :, 1:2])


def probs(scores, ok):
    s = jnp.where(ok[None], scores.reshape(-1, ok.shape[0], ok.shape[1]), -1e30)
    e = jnp.exp2((s - jnp.max(s, axis=-1, keepdims=True)) * (SCALE * LOG2E))
    return e * (1.0 / jnp.sum(e, axis=-1, keepdims=True))


def keys_values(kr_ref, kv_ref, b):
    kv = jnp.concatenate([token_rows(kr_ref, b), token_rows(kv_ref, b)], axis=0)
    return kv[:, :HEAD_DIM], kv[:, HEAD_DIM:]


def attn_fwd_kernel(q_ref, kv_ref, kr_ref, qi_ref, ki_ref, *refs):
    o_ref = refs[-1]
    shape = (o_ref.shape[0], o_ref.shape[2], HEAD_DIM)
    batch = range(q_ref.shape[1])
    kv = [keys_values(kr_ref, kv_ref, b) for b in batch]
    scores = [dot(by_head(token_rows(q_ref, b)), kv[b][0], NT) for b in batch]
    for b in batch:
        ok = allowed_block(qi_ref, ki_ref, b)
        toks = ok.shape[0]
        o = dot(probs(scores[b], ok).astype(BF16).reshape(scores[b].shape), kv[b][1], NN).astype(BF16)
        for h in range(o.shape[0] // toks):
            o_ref[:, b, :, h * HEAD_DIM:(h + 1) * HEAD_DIM] = o[h * toks:(h + 1) * toks].reshape(shape)


def attn_bwd_kernel(n_alias, q_ref, kv_ref, kr_ref, do0_ref, do1_ref, do2_ref, do3_ref, qi_ref, ki_ref, cos_ref, sin_ref, cosr_ref, sinr_ref, *refs):
    dq_ref, dkv_ref, dkr_ref = refs[n_alias:]
    shape = (dq_ref.shape[0], dq_ref.shape[2], HEAD_DIM)
    batch = range(q_ref.shape[1])
    kv = [keys_values(kr_ref, kv_ref, b) for b in batch]
    q = [by_head(token_rows(q_ref, b)) for b in batch]
    do = [by_head(jnp.concatenate([token_rows(d, b) for d in (do0_ref, do1_ref, do2_ref, do3_ref)], axis=0)) for b in batch]
    scores = [dot(q[b], kv[b][0], NT) for b in batch]
    grad_probs = [dot(do[b], kv[b][1], NT) for b in batch]
    low, ds = [], []
    for b in batch:
        p = probs(scores[b], allowed_block(qi_ref, ki_ref, b))
        dp = grad_probs[b].reshape(p.shape)
        low.append(p.astype(BF16).reshape(scores[b].shape))
        ds.append((p * (dp - jnp.sum(p * dp, axis=-1, keepdims=True))).astype(BF16).reshape(scores[b].shape))
    for b in batch:
        toks = kv[b][0].shape[0] // 2
        dv = dot(low[b], do[b], TN)
        dk = dot(ds[b], q[b], TN) * SCALE
        dq = dot(ds[b], kv[b][0], NN) * SCALE
        cos, sin = token_rows(cos_ref, b), token_rows(sin_ref, b)
        for h in range(dq.shape[0] // toks):
            part = dq[h * toks:(h + 1) * toks]
            dq_ref[:, b, :, h * HEAD_DIM:(h + 1) * HEAD_DIM] = (part * cos - swap_pairs(part) * sin).astype(BF16).reshape(shape)
        dk_r, dk_l = dk[:toks], dk[toks:]
        dkv_ref[:, b, :, :HEAD_DIM] = (dk_l * cos - swap_pairs(dk_l) * sin).reshape(shape)
        dkv_ref[:, b, :, HEAD_DIM:] = dv[toks:].reshape(shape)
        dkr_ref[:, b, :, :HEAD_DIM] = (dk_r * token_rows(cosr_ref, b) - swap_pairs(dk_r) * token_rows(sinr_ref, b)).astype(BF16).reshape(shape)
        dkr_ref[:, b, :, HEAD_DIM:] = dv[:toks].astype(BF16).reshape(shape)


FWD_ROWS, BWD_ROWS = 4, 2


def block_at(count, pieces, span, width, col):
    return pl.BlockSpec((pieces, count, span, width), lambda b: (0, b, 0, col))


def attn_specs(count, group, q_cols, pieces, span):
    toks = pieces * span
    s, t = SLOT[group], SLOT[group ^ 2]
    kv_cols = 2 * HEAD_DIM
    return ([block_at(count, pieces, span, q_cols, s), block_at(count, pieces, span, kv_cols, s % 2), block_at(count, pieces, span, kv_cols, t % 2)],
            [pl.BlockSpec((count, toks, 2), lambda b: (b, 0, 0)), pl.BlockSpec((1, 2 * toks), lambda b: (0, 0))])


def attn_forward(group, q, kv, kvr, qinfo, kinfo, buf):
    pieces, rows, span, q_all = q.shape
    q_cols, toks = q_all // 4, pieces * span
    big, info = attn_specs(FWD_ROWS, group, q_cols, pieces, span)
    ops, specs, alias = (q, kv, kvr, qinfo, kinfo), big + info, {}
    if buf is not None:
        ops, specs, alias = ops + (buf,), specs + [ANY], {5: 0}
    return pl.pallas_call(
        attn_fwd_kernel, grid=(rows // FWD_ROWS,), in_specs=specs, out_specs=block_at(FWD_ROWS, pieces, span, q_cols, SLOT[group]),
        out_shape=jax.ShapeDtypeStruct(q.shape, BF16), input_output_aliases=alias,
        compiler_params=pltpu.CompilerParams(vmem_limit_bytes=VMEM_LIMIT),
        cost_estimate=cost(8 * rows * toks * toks * q_cols, 8 * rows * toks * q_cols), name="attn_fwd")(*ops)


def attn_backward(group, q, kv, kvr, dos, qinfo, kinfo, tabs, bufs):
    pieces, rows, span, q_all = q.shape
    q_cols, toks, s = q_all // 4, pieces * span, SLOT[group]
    kv_cols = 2 * HEAD_DIM
    big, info = attn_specs(BWD_ROWS, group, q_cols, pieces, span)
    do_spec = pl.BlockSpec((BWD_ROWS, span, q_cols), lambda b: (b, 0, s))
    ops = (q, kv, kvr, *dos, qinfo, kinfo, *tabs)
    specs, alias = big + [do_spec] * 4 + info + [block_at(BWD_ROWS, pieces, span, HEAD_DIM, 0)] * 4, {}
    n_alias = 0
    for i, buf in enumerate(bufs):
        if buf is not None:
            alias[len(ops)] = i
            ops, specs, n_alias = ops + (buf,), specs + [ANY], n_alias + 1
    half = (pieces, rows, span, 2 * kv_cols)
    return pl.pallas_call(
        functools.partial(attn_bwd_kernel, n_alias), grid=(rows // BWD_ROWS,), in_specs=specs,
        out_specs=[block_at(BWD_ROWS, pieces, span, q_cols, s), block_at(BWD_ROWS, pieces, span, kv_cols, s % 2), block_at(BWD_ROWS, pieces, span, kv_cols, s % 2)],
        out_shape=[jax.ShapeDtypeStruct(q.shape, BF16), jax.ShapeDtypeStruct(half, F32), jax.ShapeDtypeStruct(half, BF16)],
        input_output_aliases=alias, compiler_params=pltpu.CompilerParams(vmem_limit_bytes=VMEM_LIMIT),
        cost_estimate=cost(20 * rows * toks * toks * q_cols, 20 * rows * toks * q_cols), name="attn_bwd")(*ops)


def grad_in_kernel(dq_ref, da_ref, db_ref, wq_ref, wkv_ref, *outs):
    half = da_ref.shape[1]
    out = dot(dq_ref[...], wq_ref[...], NT) + dot(da_ref[...], wkv_ref[:, :half], NT) + dot(db_ref[...], wkv_ref[:, half:], NT)
    rows = out.shape[0] // len(outs)
    for i, ref in enumerate(outs):
        ref[...] = out[i * rows:(i + 1) * rows].astype(ref.dtype)


def grad_in(dq, da, db, wq, wkv, at, types):
    count, width = len(types), wq.shape[0]
    rows, tile = dq.shape[0] // 4, 4 * HEAD_DIM
    part = lambda a: pl.BlockSpec((count * rows, a.shape[1]), lambda n: (at, 0))
    row = lambda a: pl.BlockSpec((tile, a.shape[1]), lambda n: (n, 0))
    return pl.pallas_call(
        grad_in_kernel, grid=(width // tile,), in_specs=[part(dq), part(da), part(db), row(wq), row(wkv)],
        out_specs=[pl.BlockSpec((rows, tile), lambda n: (0, n))] * count,
        out_shape=[jax.ShapeDtypeStruct((rows, width), t) for t in types],
        compiler_params=pltpu.CompilerParams(vmem_limit_bytes=VMEM_LIMIT),
        cost_estimate=cost(2 * count * rows * width * (wq.shape[1] + wkv.shape[1]), 4 * count * rows * width), name="grad_in")(dq, da, db, wq, wkv)


def head_out_kernel(h_ref, w_ref, first_ref, second_ref):
    out = dot(h_ref[...], w_ref[...], NN)
    rows = first_ref.shape[0]
    first_ref[...] = out[:rows].astype(first_ref.dtype)
    second_ref[...] = out[rows:].astype(second_ref.dtype)


def head_out(heads, w, pair_at, types):
    rows, inner, width, tile = heads.shape[0] // 2, heads.shape[1], w.shape[1], 4 * HEAD_DIM
    out = pl.BlockSpec((rows // 2, tile), lambda n: (0, n))
    return pl.pallas_call(
        head_out_kernel, grid=(width // tile,),
        in_specs=[pl.BlockSpec((rows, inner), lambda n: (pair_at, 0)), pl.BlockSpec((inner, tile), lambda n: (0, n))], out_specs=[out, out],
        out_shape=[jax.ShapeDtypeStruct((rows // 2, width), t) for t in types],
        compiler_params=pltpu.CompilerParams(vmem_limit_bytes=VMEM_LIMIT),
        cost_estimate=cost(2 * rows * width * inner, 4 * rows * width), name="head_out")(heads, w)


def residual_kernel(x_ref, a_ref, b_ref, *refs):
    total = a_ref[...].astype(F32) + b_ref[...].astype(F32)
    refs[-1][...] = (x_ref[...].astype(F32) + total.astype(BF16).astype(F32)).astype(BF16)


def norm_back_kernel(x_ref, g_ref, a_ref, b_ref, gain_ref, *refs):
    gh_ref, part_ref = refs[-2:]
    tile, width = x_ref.shape
    chunk = 2 * HEAD_DIM
    cuts = [slice(c, c + chunk) for c in range(0, width, chunk)]

    @pl.when(pl.program_id(0) == 0)
    def _():
        part_ref[...] = jnp.zeros_like(part_ref)

    def load(cols):
        return x_ref[:, cols].astype(F32), a_ref[:, cols].astype(F32) + b_ref[:, cols].astype(F32)

    square, cross = jnp.zeros((tile, chunk), F32), jnp.zeros((tile, chunk), F32)
    for cols in cuts:
        x, gn = load(cols)
        square += x * x
        cross += gn * gain_ref[:, cols] * x
    inv = lax.rsqrt(jnp.sum(square, axis=-1, keepdims=True) / width + NORM_EPS)
    slope = inv * inv * inv * (jnp.sum(cross, axis=-1, keepdims=True) / width)
    for cols in cuts:
        x, gn = load(cols)
        scaled = gn * inv
        gh_ref[:, cols] = (g_ref[:, cols].astype(F32) + (scaled * gain_ref[:, cols] - x * slope)).astype(BF16)
        part_ref[:, cols] += jnp.sum((scaled * x).reshape(-1, 8, chunk), axis=0)


def half_rows_call(kernel, half, arrays, gain, buf, out_shape, with_part):
    rows, width = arrays[-1].shape
    steps = 4 if with_part else 2
    tile = rows // steps
    mine = pl.BlockSpec((tile, width), lambda m, h: (m, 0))
    full = pl.BlockSpec((tile, width), lambda m, h: (h[0] * steps + m, 0))
    specs = [full if a.shape[0] == out_shape[0] else mine for a in arrays]
    ops, alias = tuple(arrays), {}
    if gain is not None:
        ops, specs = ops + (gain,), specs + [pl.BlockSpec(gain.shape, lambda m, h: (0, 0))]
    if buf is not None:
        alias = {1 + len(ops): 0}
        ops, specs = ops + (buf,), specs + [ANY]
    outs, out_specs = [jax.ShapeDtypeStruct(out_shape, BF16)], [full]
    if with_part:
        outs.append(jax.ShapeDtypeStruct((8, width), F32))
        out_specs.append(pl.BlockSpec((8, width), lambda m, h: (0, 0)))

    def body(h_ref, *refs):
        kernel(*refs)

    return pl.pallas_call(
        body, grid_spec=pltpu.PrefetchScalarGridSpec(num_scalar_prefetch=1, grid=(steps,), in_specs=specs, out_specs=out_specs),
        out_shape=outs, input_output_aliases=alias, cost_estimate=cost(1000 * rows * width, 10 * rows * width))(half, *ops)


def solution(mesh):
    tp = mesh.shape['tp']
    chips = tp // 2
    mirror = [2 * (chips - 1 - i // 2) + i % 2 for i in range(tp)]
    mates = [[(i, i ^ r) for i in range(tp)] for r in range(4)]
    far = [[(mirror[i] ^ r, i) for i in range(tp)] for r in range(4)]
    pair = list(enumerate(mirror))
    later = [(i, j) for i, j in pair if i < j]
    earlier = [(i, j) for i, j in pair if i > j]

    def send(x, perm):
        return lax.ppermute(x, 'tp', perm)

    def device_step(hidden, positions, doc_ids, norm_gain, w_query, w_key, w_value, w_out, grad_out):
        last = []

        def run(fn, *args):
            if last:
                *args, _ = lax.optimization_barrier((*args, last[0]))
            out = fn(*args)
            last[:] = [jax.tree.leaves(out)[0]]
            return out

        def after(x):
            return lax.optimization_barrier((x, last[0]))[0]

        me = lax.axis_index('tp')
        core = me % 2
        all_rows, span, width = hidden.shape
        rows = all_rows // 2
        toks, half = 4 * span, rows * span
        q_cols = w_query.shape[1]
        split = lambda x: (lax.dynamic_slice_in_dim(x, core * rows, rows), lax.dynamic_slice_in_dim(x, (1 - core) * rows, rows))
        four = lambda x: x.reshape(4, rows, span, x.shape[-1])
        flat = lambda x: x.reshape(-1, x.shape[-1])

        hid_mine, hid_other = split(hidden)
        hid2 = send(hid_mine, mates[2])
        hid1 = send(hid_other, mates[1])
        w_kv = jnp.concatenate([w_key, w_value], axis=1)
        wkv2 = send(w_kv, pair)
        wkv1 = send(w_kv, mates[1])
        wq1 = send(w_query, mates[1])
        pos_mine, pos_other = split(positions)
        by_piece = (pos_mine, pos_other, pos_mine, pos_other)
        pos_loc = [pos_mine] + [send(by_piece[p], mates[p]) for p in (1, 2, 3)]
        pos_rem = [send(by_piece[p], far[p]) for p in range(4)]
        wq2 = send(w_query, pair)
        hid3 = send(hid_other, mates[3])
        wo1 = send(w_out, mates[1])
        wo2 = send(w_out, pair)
        g_mine, g_other = split(grad_out)
        grd1 = send(g_other, mates[1])
        grd2 = send(g_mine, mates[2])
        grd3 = send(g_other, mates[3])

        gain_row = norm_gain.astype(F32)[None]

        def put(x, buf, at, axis, normalize=False):
            if buf is None:
                return run(lambda x_: place(x_, gain_row, None, at, axis, normalize), x)
            return run(lambda x_, b: place(x_, gain_row, b, at, axis, normalize), x, buf)

        wq_all = put(w_query, None, SLOT[0], 1)
        wkv_all = put(w_kv, None, SLOT[0], 1)
        wo_all = put(w_out, None, SLOT[0], 0)
        normed = put(flat(hid_mine), None, 0, 0, True)
        grads = put(flat(g_mine), None, 0, 0)
        normed = put(flat(hid1), normed, 1, 0, True)
        wkv_all = put(wkv1, wkv_all, SLOT[1], 1)
        wq_all = put(wq1, wq_all, SLOT[1], 1)
        wo_all = put(wo1, wo_all, SLOT[1], 0)
        grads = put(flat(grd1), grads, 1, 0)
        wkv3 = send(after(wkv2), mates[1])
        wkv_all = put(wkv2, wkv_all, SLOT[2], 1)
        wkv_all = put(wkv3, wkv_all, SLOT[3], 1)
        normed = put(flat(hid2), normed, 2, 0, True)

        pos_loc, pos_rem = jnp.stack(pos_loc), jnp.stack(pos_rem)
        pos_loc, pos_rem = after((pos_loc, pos_rem))
        idx_of = lambda dev: (jnp.stack([dev ^ p for p in range(4)])[:, None] * span + jnp.arange(span)).astype(jnp.int32)
        q_idx, r_idx = idx_of(me), idx_of(2 * (chips - 1 - me // 2) + core)
        q_full = jnp.broadcast_to(q_idx[:, None, :], pos_loc.shape)
        qinfo = jnp.stack([q_full, q_full - pos_loc], axis=-1)
        qinfo = jnp.moveaxis(qinfo, 1, 0).reshape(rows, toks, 2)
        kinfo = jnp.concatenate([r_idx.reshape(1, toks), q_idx.reshape(1, toks)], axis=1)
        inv_freq = ROPE_BASE ** (-jnp.arange(0, HEAD_DIM, 2, dtype=F32) / HEAD_DIM)
        lane_freq = jnp.repeat(inv_freq, 2)
        lane_sign = jnp.where(jnp.arange(HEAD_DIM) % 2 == 0, -1.0, 1.0).astype(F32)

        def tables(pos):
            ang = pos.astype(F32)[..., None] * lane_freq
            return jnp.cos(ang), jnp.sin(ang) * lane_sign

        cos_l, sin_l = tables(pos_loc)
        cos_r, sin_r = tables(pos_rem)
        cos2, sin2 = flat(cos_l), flat(sin_l)
        cos2, sin2, qinfo, kinfo, cos_r, sin_r = lax.optimization_barrier((cos2, sin2, qinfo, kinfo, cos_r, sin_r))
        last[:] = [cos2]
        tabs = (four(cos2), four(sin2), cos_r, sin_r)

        early = [run(lambda x, w: project(x, w, cos2, sin2, 2 * i, 2, 1, (0, 3 * half)), normed, wkv_all) for i in range(2)]
        wq3 = send(after(wq2), mates[1])
        wq_all = put(wq2, wq_all, SLOT[2], 1)
        wq_all = put(wq3, wq_all, SLOT[3], 1)
        normed = put(flat(hid3), normed, 3, 0, True)

        kvs, kv_in = [], []
        for i in range(2):
            kv = four(run(lambda x, w, e: project(x, w, cos2, sin2, 2 * i, 2, 1, (3, half), e), normed, wkv_all, early[i]))
            kvs.append(kv)
            kv_in.append(send(kv, later))
        q_all = four(run(lambda x, w: project(x, w, cos2, sin2, 0, 2 * q_cols // HEAD_DIM, 2), normed, wq_all))
        wo3 = send(after(wo2), mates[1])
        wo_all = put(wo2, wo_all, SLOT[2], 0)
        wo_all = put(wo3, wo_all, SLOT[3], 0)
        head_grad = lambda g, w: dot(g, w, NT).astype(BF16).reshape(rows, span, -1)
        dos = [run(head_grad, flat(g), wo_all) for g in (g_mine, grd1, grd2)]
        grads = put(flat(grd2), grads, 2, 0)
        heads = None
        for g in GROUPS:
            local, far_in = kvs[SLOT[g] // 2], kv_in[SLOT[g ^ 2] // 2]
            if heads is None:
                heads = run(lambda q, kv, kr: attn_forward(g, q, kv, kr, qinfo, kinfo, None), q_all, local, far_in)
            else:
                if SLOT[g] == 2:
                    grads = put(flat(grd3), grads, 3, 0)
                heads = run(lambda q, kv, kr, h: attn_forward(g, q, kv, kr, qinfo, kinfo, h), q_all, local, far_in, heads)
        heads_flat = flat(heads)
        att = [None] * 4
        out2, out3 = run(lambda h, w: head_out(h, w, 1, (BF16, BF16)), heads_flat, wo_all)
        att[2], att[3] = send(out2, mates[2]), send(out3, mates[3])
        own_out, out1 = run(lambda h, w: head_out(h, w, 0, (F32, BF16)), heads_flat, wo_all)
        att[1] = send(out1, mates[1])

        dos.append(run(head_grad, flat(grd3), wo_all))
        dq, dkv, dkr, dkv_in = None, [None, None], [None, None], [None, None]
        for g in GROUPS:
            i = SLOT[g] // 2
            bufs = [b for b in (dq, dkv[i], dkr[i]) if b is not None]
            given = tuple(b is not None for b in (dq, dkv[i], dkr[i]))

            def fn(q, kv, kr, d0, d1, d2, d3, *rest):
                it = iter(rest)
                return attn_backward(g, q, kv, kr, (d0, d1, d2, d3), qinfo, kinfo, tabs, [next(it) if ok else None for ok in given])

            dq, dkv[i], dkr[i] = run(fn, q_all, kvs[i], kv_in[SLOT[g ^ 2] // 2], *dos, *bufs)
            if SLOT[g] % 2 == 1:
                dkv_in[i] = send(dkr[i], earlier)

        def add_far(mine, theirs):
            swapped = jnp.concatenate([theirs[..., 2 * HEAD_DIM:], theirs[..., :2 * HEAD_DIM]], axis=-1)
            return flat((mine + swapped.astype(F32)).astype(BF16))

        cut = lambda x, s, n: x[:, s * q_cols:(s + n) * q_cols]
        low = lambda x: x.astype(BF16)
        kv_half = 2 * HEAD_DIM
        dq_flat = flat(dq)
        spq13 = send(run(lambda d, n: low(dot(n, cut(d, 0, 2), TN)), dq_flat, normed), mates[1])
        dkv_a = run(add_far, dkv[0], dkv_in[0])
        spk13 = send(run(lambda d, n: low(dot(n, d, TN)), dkv_a, normed), mates[1])
        spq2 = send(run(lambda d, n, e: low(dot(n, cut(d, 3, 1), TN) + e[:, q_cols:].astype(F32)), dq_flat, normed, spq13), pair)
        so13 = send(run(lambda h, g: low(dot(cut(h, 0, 2), g, TN)), heads_flat, grads), mates[1])
        dkv_b = run(add_far, dkv[1], dkv_in[1])
        gn = [None] * 4
        for p in (2, 3):
            gn[p] = send(run(lambda *x: grad_in(*x, p, (BF16,))[0], dq_flat, dkv_a, dkv_b, wq_all, wkv_all), mates[p])
        gn2, gn3 = gn[2], gn[3]
        so1, so3 = run(lambda e: (e[:q_cols], e[q_cols:]), so13)
        so2 = send(run(lambda h, gg, e: low(dot(cut(h, 3, 1), gg, TN) + e.astype(F32)), heads_flat, grads, so3), pair)
        spk2 = send(run(lambda d, n, e: low(dot(n, d[:, kv_half:], TN) + e[:, kv_half:].astype(F32)), dkv_b, normed, spk13), pair)
        mine_half, other_half = core.astype(jnp.int32)[None], (1 - core).astype(jnp.int32)[None]
        flat_shape = (all_rows * span, width)
        hid_flat, g_flat = flat(hidden), flat(grad_out)
        own_in, gn1 = run(lambda d, a, b, wq, wk: grad_in(d, a, b, wq, wk, 0, (F32, BF16)), dq_flat, dkv_a, dkv_b, wq_all, wkv_all)
        gn1 = send(gn1, mates[1])
        attn_out = run(lambda x, a, b: half_rows_call(residual_kernel, mine_half, (x, a, b), None, None, flat_shape, False)[0], hid_flat, own_out, flat(att[2]))
        attn_out = run(lambda x, a, b, o: half_rows_call(residual_kernel, other_half, (x, a, b), None, o, flat_shape, False)[0], hid_flat, flat(att[1]), flat(att[3]), attn_out)
        back_call = lambda h, arrays, buf: half_rows_call(norm_back_kernel, h, arrays, gain_row, buf, flat_shape, True)
        grad_hidden, part_a = run(lambda x, g, a, b: back_call(mine_half, (x, g, a, b), None), hid_flat, g_flat, own_in, gn2)
        dwq = run(lambda d, n, e, f: dot(n, cut(d, 2, 1), TN) + (e[:, :q_cols].astype(F32) + f.astype(F32)), dq_flat, normed, spq13, spq2)
        own_kv = after(run(lambda d, n, e: dot(n, d[:, :kv_half], TN) + e[:, :kv_half].astype(F32), dkv_b, normed, spk13))
        dwo = run(lambda h, g, a, b: dot(cut(h, 2, 1), g, TN) + (a.astype(F32) + b.astype(F32)), heads_flat, grads, so1, so2)
        grad_hidden, part_b = run(lambda x, g, a, b, o: back_call(other_half, (x, g, a, b), o), hid_flat, g_flat, gn1, gn3, grad_hidden)
        gain_sum = jnp.sum(part_a + part_b, axis=0).reshape(-1, HEAD_DIM)
        for perm in (mates[1], mates[2], pair):
            gain_sum = gain_sum + send(gain_sum, perm)
        dwk = own_kv[:, :HEAD_DIM] + spk2[:, :HEAD_DIM].astype(F32)
        dwv = own_kv[:, HEAD_DIM:] + spk2[:, HEAD_DIM:].astype(F32)
        return attn_out.reshape(hidden.shape), grad_hidden.reshape(hidden.shape), gain_sum.reshape(-1), dwq, dwk, dwv, dwo

    row_spec = P('dp', 'tp', None)
    tok_spec = P('dp', 'tp')
    col_spec = P(None, 'tp')
    return jax.shard_map(
        device_step, mesh=mesh,
        in_specs=(row_spec, tok_spec, tok_spec, P(), col_spec, col_spec, col_spec, P('tp', None), row_spec),
        out_specs=(row_spec, row_spec, P('dp'), P('dp', 'tp'), P('dp', 'tp'), P('dp', 'tp'), P(('dp', 'tp'), None)),
        check_vma=False)
```

```python
import functools

import jax
import jax.numpy as jnp
from jax import lax
from jax.experimental import pallas as pl
from jax.experimental.pallas import tpu as pltpu
from jax.sharding import PartitionSpec as P


HEAD_DIM = 128
NORM_EPS = 1e-5
ROPE_BASE = 10000.0
SCALE = HEAD_DIM ** -0.5
LOG2E = 1.4426950408889634
F32 = jnp.float32
BF16 = jnp.bfloat16
NN = (((1,), (0,)), ((), ()))
NT = (((1,), (1,)), ((), ()))
TN = (((0,), (0,)), ((), ()))
VMEM_LIMIT = 63000 * 1024
GROUPS = (1, 3, 0, 2)
SLOT = {g: s for s, g in enumerate(GROUPS)}
ANY = pl.BlockSpec(memory_space=pl.ANY)


def dot(a, b, dims):
    return lax.dot_general(a, b, dims, preferred_element_type=F32)


def cost(flops, size):
    return pl.CostEstimate(flops=int(flops), bytes_accessed=int(size), transcendentals=0)


def swap_pairs(x):
    lane = lax.broadcasted_iota(jnp.int32, x.shape, 1)
    return jnp.where(lane % 2 == 0, pltpu.roll(x, HEAD_DIM - 1, 1), pltpu.roll(x, 1, 1))


def place_kernel(normalize, x_ref, gain_ref, *refs):
    x = x_ref[...]
    if normalize:
        xf = x.astype(F32)
        inv = lax.rsqrt(jnp.mean(xf * xf, axis=-1, keepdims=True) + NORM_EPS)
        x = (xf * inv * gain_ref[...]).astype(BF16)
    refs[-1][...] = x


def place(x, gain, buf, at, axis, normalize=False):
    rows, width = x.shape
    steps = 2
    tile = rows // steps
    shape = (4 * rows, width) if axis == 0 else (rows, 4 * width)
    where = (lambda m: (at * steps + m, 0)) if axis == 0 else (lambda m: (m, at))
    ops, specs, alias = (x, gain), [pl.BlockSpec((tile, width), lambda m: (m, 0)), pl.BlockSpec(gain.shape, lambda m: (0, 0))], {}
    if buf is not None:
        ops, specs, alias = ops + (buf,), specs + [ANY], {2: 0}
    return pl.pallas_call(
        functools.partial(place_kernel, normalize), grid=(steps,), in_specs=specs, out_specs=pl.BlockSpec((tile, width), where),
        out_shape=jax.ShapeDtypeStruct(shape, BF16), input_output_aliases=alias,
        cost_estimate=cost(1000 * rows * width, 4 * rows * width), name="place")(*ops)


def proj_kernel(turned, chunk, x_ref, w_ref, cos_ref, sin_ref, *refs):
    o_ref = refs[-1]
    for m in range(0, x_ref.shape[0], chunk):
        rows = slice(m, m + chunk)
        acc = dot(x_ref[rows], w_ref[...], NN)
        for h in range(acc.shape[1] // HEAD_DIM):
            cols = slice(h * HEAD_DIM, (h + 1) * HEAD_DIM)
            part = acc[:, cols]
            if h < turned:
                part = part * cos_ref[rows] + swap_pairs(part) * sin_ref[rows]
            o_ref[rows, cols] = part.astype(BF16)


def project(x, w, cos, sin, first, count, turned, span=None, buf=None):
    rows, width = x.shape
    tile, chunk = 2 * HEAD_DIM, rows // 4
    at, part = span or (0, rows)
    some = lambda a: pl.BlockSpec((part, a.shape[1]), lambda n: (at, 0))
    ops, alias = (x, w, cos, sin), {}
    specs = [some(x), pl.BlockSpec((width, tile), lambda n: (0, first + n)), some(cos), some(sin)]
    if buf is not None:
        alias = {len(ops): 0}
        ops, specs = ops + (buf,), specs + [ANY]
    return pl.pallas_call(
        functools.partial(proj_kernel, turned, chunk), grid=(count,), in_specs=specs,
        out_specs=pl.BlockSpec((part, tile), lambda n: (at, n)), input_output_aliases=alias,
        out_shape=jax.ShapeDtypeStruct((rows, count * tile), BF16),
        compiler_params=pltpu.CompilerParams(vmem_limit_bytes=VMEM_LIMIT),
        cost_estimate=cost(2 * part * width * count * tile, 2 * part * width), name="project")(*ops)


def token_rows(ref, b):
    x = ref[:, b] if len(ref.shape) == 4 else ref[b]
    return x.reshape(-1, x.shape[-1])


def by_head(x):
    return jnp.concatenate([x[:, h * HEAD_DIM:(h + 1) * HEAD_DIM] for h in range(x.shape[1] // HEAD_DIM)], axis=0)


def allowed_block(qi_ref, ki_ref, b):
    kidx = ki_ref[...]
    return (kidx <= qi_ref[b, :, 0:1]) & (kidx >= qi_ref[b, :, 1:2])


def probs(scores, ok):
    s = jnp.where(ok[None], scores.reshape(-1, ok.shape[0], ok.shape[1]), -1e30)
    e = jnp.exp2((s - jnp.max(s, axis=-1, keepdims=True)) * (SCALE * LOG2E))
    return e * (1.0 / jnp.sum(e, axis=-1, keepdims=True))


def keys_values(kr_ref, kv_ref, b):
    kv = jnp.concatenate([token_rows(kr_ref, b), token_rows(kv_ref, b)], axis=0)
    return kv[:, :HEAD_DIM], kv[:, HEAD_DIM:]


def attn_fwd_kernel(q_ref, kv_ref, kr_ref, qi_ref, ki_ref, *refs):
    o_ref = refs[-1]
    shape = (o_ref.shape[0], o_ref.shape[2], HEAD_DIM)
    batch = range(q_ref.shape[1])
    kv = [keys_values(kr_ref, kv_ref, b) for b in batch]
    scores = [dot(by_head(token_rows(q_ref, b)), kv[b][0], NT) for b in batch]
    for b in batch:
        ok = allowed_block(qi_ref, ki_ref, b)
        toks = ok.shape[0]
        o = dot(probs(scores[b], ok).astype(BF16).reshape(scores[b].shape), kv[b][1], NN).astype(BF16)
        for h in range(o.shape[0] // toks):
            o_ref[:, b, :, h * HEAD_DIM:(h + 1) * HEAD_DIM] = o[h * toks:(h + 1) * toks].reshape(shape)


def attn_bwd_kernel(n_alias, q_ref, kv_ref, kr_ref, do0_ref, do1_ref, do2_ref, do3_ref, qi_ref, ki_ref, cos_ref, sin_ref, cosr_ref, sinr_ref, *refs):
    dq_ref, dkv_ref, dkr_ref = refs[n_alias:]
    shape = (dq_ref.shape[0], dq_ref.shape[2], HEAD_DIM)
    batch = range(q_ref.shape[1])
    kv = [keys_values(kr_ref, kv_ref, b) for b in batch]
    q = [by_head(token_rows(q_ref, b)) for b in batch]
    do = [by_head(jnp.concatenate([token_rows(d, b) for d in (do0_ref, do1_ref, do2_ref, do3_ref)], axis=0)) for b in batch]
    scores = [dot(q[b], kv[b][0], NT) for b in batch]
    grad_probs = [dot(do[b], kv[b][1], NT) for b in batch]
    low, ds = [], []
    for b in batch:
        p = probs(scores[b], allowed_block(qi_ref, ki_ref, b))
        dp = grad_probs[b].reshape(p.shape)
        low.append(p.astype(BF16).reshape(scores[b].shape))
        ds.append((p * (dp - jnp.sum(p * dp, axis=-1, keepdims=True))).astype(BF16).reshape(scores[b].shape))
    for b in batch:
        toks = kv[b][0].shape[0] // 2
        dv = dot(low[b], do[b], TN)
        dk = dot(ds[b], q[b], TN) * SCALE
        dq = dot(ds[b], kv[b][0], NN) * SCALE
        cos, sin = token_rows(cos_ref, b), token_rows(sin_ref, b)
        for h in range(dq.shape[0] // toks):
            part = dq[h * toks:(h + 1) * toks]
            dq_ref[:, b, :, h * HEAD_DIM:(h + 1) * HEAD_DIM] = (part * cos - swap_pairs(part) * sin).astype(BF16).reshape(shape)
        dk_r, dk_l = dk[:toks], dk[toks:]
        dkv_ref[:, b, :, :HEAD_DIM] = (dk_l * cos - swap_pairs(dk_l) * sin).reshape(shape)
        dkv_ref[:, b, :, HEAD_DIM:] = dv[toks:].reshape(shape)
        dkr_ref[:, b, :, :HEAD_DIM] = (dk_r * token_rows(cosr_ref, b) - swap_pairs(dk_r) * token_rows(sinr_ref, b)).astype(BF16).reshape(shape)
        dkr_ref[:, b, :, HEAD_DIM:] = dv[:toks].astype(BF16).reshape(shape)


FWD_ROWS, BWD_ROWS = 4, 2


def block_at(count, pieces, span, width, col):
    return pl.BlockSpec((pieces, count, span, width), lambda b: (0, b, 0, col))


def attn_specs(count, group, q_cols, pieces, span):
    toks = pieces * span
    s, t = SLOT[group], SLOT[group ^ 2]
    kv_cols = 2 * HEAD_DIM
    return ([block_at(count, pieces, span, q_cols, s), block_at(count, pieces, span, kv_cols, s % 2), block_at(count, pieces, span, kv_cols, t % 2)],
            [pl.BlockSpec((count, toks, 2), lambda b: (b, 0, 0)), pl.BlockSpec((1, 2 * toks), lambda b: (0, 0))])


def attn_forward(group, q, kv, kvr, qinfo, kinfo, buf):
    pieces, rows, span, q_all = q.shape
    q_cols, toks = q_all // 4, pieces * span
    big, info = attn_specs(FWD_ROWS, group, q_cols, pieces, span)
    ops, specs, alias = (q, kv, kvr, qinfo, kinfo), big + info, {}
    if buf is not None:
        ops, specs, alias = ops + (buf,), specs + [ANY], {5: 0}
    return pl.pallas_call(
        attn_fwd_kernel, grid=(rows // FWD_ROWS,), in_specs=specs, out_specs=block_at(FWD_ROWS, pieces, span, q_cols, SLOT[group]),
        out_shape=jax.ShapeDtypeStruct(q.shape, BF16), input_output_aliases=alias,
        compiler_params=pltpu.CompilerParams(vmem_limit_bytes=VMEM_LIMIT),
        cost_estimate=cost(8 * rows * toks * toks * q_cols, 8 * rows * toks * q_cols), name="attn_fwd")(*ops)


def attn_backward(group, q, kv, kvr, dos, qinfo, kinfo, tabs, bufs):
    pieces, rows, span, q_all = q.shape
    q_cols, toks, s = q_all // 4, pieces * span, SLOT[group]
    kv_cols = 2 * HEAD_DIM
    big, info = attn_specs(BWD_ROWS, group, q_cols, pieces, span)
    do_spec = pl.BlockSpec((BWD_ROWS, span, q_cols), lambda b: (b, 0, s))
    ops = (q, kv, kvr, *dos, qinfo, kinfo, *tabs)
    specs, alias = big + [do_spec] * 4 + info + [block_at(BWD_ROWS, pieces, span, HEAD_DIM, 0)] * 4, {}
    n_alias = 0
    for i, buf in enumerate(bufs):
        if buf is not None:
            alias[len(ops)] = i
            ops, specs, n_alias = ops + (buf,), specs + [ANY], n_alias + 1
    half = (pieces, rows, span, 2 * kv_cols)
    return pl.pallas_call(
        functools.partial(attn_bwd_kernel, n_alias), grid=(rows // BWD_ROWS,), in_specs=specs,
        out_specs=[block_at(BWD_ROWS, pieces, span, q_cols, s), block_at(BWD_ROWS, pieces, span, kv_cols, s % 2), block_at(BWD_ROWS, pieces, span, kv_cols, 0)],
        out_shape=[jax.ShapeDtypeStruct(q.shape, BF16), jax.ShapeDtypeStruct(half, F32), jax.ShapeDtypeStruct((pieces, rows, span, kv_cols), BF16)],
        input_output_aliases=alias, compiler_params=pltpu.CompilerParams(vmem_limit_bytes=VMEM_LIMIT),
        cost_estimate=cost(20 * rows * toks * toks * q_cols, 20 * rows * toks * q_cols), name="attn_bwd")(*ops)


def grad_in_kernel(dq_ref, da_ref, db_ref, wq_ref, wkv_ref, *outs):
    half = da_ref.shape[1]
    out = dot(dq_ref[...], wq_ref[...], NT) + dot(da_ref[...], wkv_ref[:, :half], NT) + dot(db_ref[...], wkv_ref[:, half:], NT)
    rows = out.shape[0] // len(outs)
    for i, ref in enumerate(outs):
        ref[...] = out[i * rows:(i + 1) * rows].astype(ref.dtype)


def grad_in(dq, da, db, wq, wkv, at, types):
    count, width = len(types), wq.shape[0]
    rows, tile = dq.shape[0] // 4, 4 * HEAD_DIM
    part = lambda a: pl.BlockSpec((count * rows, a.shape[1]), lambda n: (at, 0))
    row = lambda a: pl.BlockSpec((tile, a.shape[1]), lambda n: (n, 0))
    return pl.pallas_call(
        grad_in_kernel, grid=(width // tile,), in_specs=[part(dq), part(da), part(db), row(wq), row(wkv)],
        out_specs=[pl.BlockSpec((rows, tile), lambda n: (0, n))] * count,
        out_shape=[jax.ShapeDtypeStruct((rows, width), t) for t in types],
        compiler_params=pltpu.CompilerParams(vmem_limit_bytes=VMEM_LIMIT),
        cost_estimate=cost(2 * count * rows * width * (wq.shape[1] + wkv.shape[1]), 4 * count * rows * width), name="grad_in")(dq, da, db, wq, wkv)


def head_out_kernel(h_ref, w_ref, first_ref, second_ref):
    out = dot(h_ref[...], w_ref[...], NN)
    rows = first_ref.shape[0]
    first_ref[...] = out[:rows].astype(first_ref.dtype)
    second_ref[...] = out[rows:].astype(second_ref.dtype)


def head_out(heads, w, pair_at, types):
    rows, inner, width, tile = heads.shape[0] // 2, heads.shape[1], w.shape[1], 4 * HEAD_DIM
    out = pl.BlockSpec((rows // 2, tile), lambda n: (0, n))
    return pl.pallas_call(
        head_out_kernel, grid=(width // tile,),
        in_specs=[pl.BlockSpec((rows, inner), lambda n: (pair_at, 0)), pl.BlockSpec((inner, tile), lambda n: (0, n))], out_specs=[out, out],
        out_shape=[jax.ShapeDtypeStruct((rows // 2, width), t) for t in types],
        compiler_params=pltpu.CompilerParams(vmem_limit_bytes=VMEM_LIMIT),
        cost_estimate=cost(2 * rows * width * inner, 4 * rows * width), name="head_out")(heads, w)


def head_out_own_kernel(half_ref, h_ref, w_ref, x_ref, far_ref, own_ref, second_ref):
    out = dot(h_ref[...], w_ref[...], NN)
    rows = second_ref.shape[0]
    total = (out[:rows] + far_ref[...].astype(F32)).astype(BF16)
    own_ref[...] = (x_ref[...].astype(F32) + total.astype(F32)).astype(BF16)
    second_ref[...] = out[rows:].astype(BF16)


def head_out_own(half, heads, w, hid, far):
    rows, inner, width, tile = heads.shape[0] // 2, heads.shape[1], w.shape[1], 4 * HEAD_DIM
    part = rows // 2
    own = pl.BlockSpec((part, tile), lambda n, h: (h[0], n))
    plain = pl.BlockSpec((part, tile), lambda n, h: (0, n))
    return pl.pallas_call(
        head_out_own_kernel,
        grid_spec=pltpu.PrefetchScalarGridSpec(
            num_scalar_prefetch=1, grid=(width // tile,),
            in_specs=[pl.BlockSpec((rows, inner), lambda n, h: (0, 0)), pl.BlockSpec((inner, tile), lambda n, h: (0, n)), own, plain],
            out_specs=[own, plain]),
        out_shape=[jax.ShapeDtypeStruct(hid.shape, BF16), jax.ShapeDtypeStruct((part, width), BF16)],
        compiler_params=pltpu.CompilerParams(vmem_limit_bytes=VMEM_LIMIT),
        cost_estimate=cost(2 * rows * width * inner, 4 * rows * width), name="head_out")(half, heads, w, hid, far)


def grad_out_kernel(h_ref, g_ref, mate_ref, own_ref, far_ref):
    out = dot(h_ref[...], g_ref[...], TN) + mate_ref[...].astype(F32)
    rows = own_ref.shape[0]
    own_ref[...] = out[:rows]
    far_ref[...] = out[rows:].astype(BF16)


def grad_out_rest(heads, grads, mate):
    toks, width, cols, tile = heads.shape[0], grads.shape[1], heads.shape[1] // 2, 8 * HEAD_DIM
    col = lambda rows: pl.BlockSpec((rows, tile), lambda n: (0, n))
    return pl.pallas_call(
        grad_out_kernel, grid=(width // tile,),
        in_specs=[pl.BlockSpec((toks, cols), lambda n: (0, 1)), col(toks), col(cols)], out_specs=[col(cols // 2), col(cols // 2)],
        out_shape=[jax.ShapeDtypeStruct((cols // 2, width), F32), jax.ShapeDtypeStruct((cols // 2, width), BF16)],
        compiler_params=pltpu.CompilerParams(vmem_limit_bytes=VMEM_LIMIT),
        cost_estimate=cost(2 * toks * cols * width, 4 * toks * width), name="grad_out")(heads, grads, mate)


def residual_kernel(x_ref, a_ref, b_ref, *refs):
    total = a_ref[...].astype(F32) + b_ref[...].astype(F32)
    refs[-1][...] = (x_ref[...].astype(F32) + total.astype(BF16).astype(F32)).astype(BF16)


def norm_back_kernel(x_ref, g_ref, a_ref, b_ref, gain_ref, *refs):
    gh_ref, part_ref = refs[-2:]
    tile, width = x_ref.shape
    chunk = 2 * HEAD_DIM
    cuts = [slice(c, c + chunk) for c in range(0, width, chunk)]

    @pl.when(pl.program_id(0) == 0)
    def _():
        part_ref[...] = jnp.zeros_like(part_ref)

    def load(cols):
        return x_ref[:, cols].astype(F32), a_ref[:, cols].astype(F32) + b_ref[:, cols].astype(F32)

    square, cross = jnp.zeros((tile, chunk), F32), jnp.zeros((tile, chunk), F32)
    for cols in cuts:
        x, gn = load(cols)
        square += x * x
        cross += gn * gain_ref[:, cols] * x
    inv = lax.rsqrt(jnp.sum(square, axis=-1, keepdims=True) / width + NORM_EPS)
    slope = inv * inv * inv * (jnp.sum(cross, axis=-1, keepdims=True) / width)
    for cols in cuts:
        x, gn = load(cols)
        scaled = gn * inv
        gh_ref[:, cols] = (g_ref[:, cols].astype(F32) + (scaled * gain_ref[:, cols] - x * slope)).astype(BF16)
        part_ref[:, cols] += jnp.sum((scaled * x).reshape(-1, 8, chunk), axis=0)


def half_rows_call(kernel, half, arrays, gain, buf, out_shape, with_part):
    rows, width = arrays[-1].shape
    steps = 4 if with_part else 2
    tile = rows // steps
    mine = pl.BlockSpec((tile, width), lambda m, h: (m, 0))
    full = pl.BlockSpec((tile, width), lambda m, h: (h[0] * steps + m, 0))
    specs = [full if a.shape[0] == out_shape[0] else mine for a in arrays]
    ops, alias = tuple(arrays), {}
    if gain is not None:
        ops, specs = ops + (gain,), specs + [pl.BlockSpec(gain.shape, lambda m, h: (0, 0))]
    if buf is not None:
        alias = {1 + len(ops): 0}
        ops, specs = ops + (buf,), specs + [ANY]
    outs, out_specs = [jax.ShapeDtypeStruct(out_shape, BF16)], [full]
    if with_part:
        outs.append(jax.ShapeDtypeStruct((8, width), F32))
        out_specs.append(pl.BlockSpec((8, width), lambda m, h: (0, 0)))

    def body(h_ref, *refs):
        kernel(*refs)

    return pl.pallas_call(
        body, grid_spec=pltpu.PrefetchScalarGridSpec(num_scalar_prefetch=1, grid=(steps,), in_specs=specs, out_specs=out_specs),
        out_shape=outs, input_output_aliases=alias, cost_estimate=cost(1000 * rows * width, 10 * rows * width))(half, *ops)


def solution(mesh):
    tp = mesh.shape['tp']
    chips = tp // 2
    mirror = [2 * (chips - 1 - i // 2) + i % 2 for i in range(tp)]
    mates = [[(i, i ^ r) for i in range(tp)] for r in range(4)]
    far = [[(mirror[i] ^ r, i) for i in range(tp)] for r in range(4)]
    pair = list(enumerate(mirror))
    later = [(i, j) for i, j in pair if i < j]
    earlier = [(i, j) for i, j in pair if i > j]

    def send(x, perm):
        return lax.ppermute(x, 'tp', perm)

    def device_step(hidden, positions, doc_ids, norm_gain, w_query, w_key, w_value, w_out, grad_out):
        last = []

        def run(fn, *args):
            if last:
                *args, _ = lax.optimization_barrier((*args, last[0]))
            out = fn(*args)
            last[:] = [jax.tree.leaves(out)[0]]
            return out

        def after(x):
            return lax.optimization_barrier((x, last[0]))[0]

        me = lax.axis_index('tp')
        core = me % 2
        all_rows, span, width = hidden.shape
        rows = all_rows // 2
        toks, half = 4 * span, rows * span
        q_cols = w_query.shape[1]
        split = lambda x: (lax.dynamic_slice_in_dim(x, core * rows, rows), lax.dynamic_slice_in_dim(x, (1 - core) * rows, rows))
        four = lambda x: x.reshape(4, rows, span, x.shape[-1])
        flat = lambda x: x.reshape(-1, x.shape[-1])

        hid_mine, hid_other = split(hidden)
        hid2 = send(hid_mine, mates[2])
        hid1 = send(hid_other, mates[1])
        w_kv = jnp.concatenate([w_key, w_value], axis=1)
        wkv2 = send(w_kv, pair)
        wkv1 = send(w_kv, mates[1])
        wq1 = send(w_query, mates[1])
        pos_mine, pos_other = split(positions)
        by_piece = (pos_mine, pos_other, pos_mine, pos_other)
        pos_loc = [pos_mine] + [send(by_piece[p], mates[p]) for p in (1, 2, 3)]
        pos_rem = [send(by_piece[p], far[p]) for p in range(4)]
        wq2 = send(w_query, pair)
        hid3 = send(hid_other, mates[3])
        wo1 = send(w_out, mates[1])
        wo2 = send(w_out, pair)
        g_mine, g_other = split(grad_out)
        grd1 = send(g_other, mates[1])
        grd2 = send(g_mine, mates[2])
        grd3 = send(g_other, mates[3])

        gain_row = norm_gain.astype(F32)[None]

        def put(x, buf, at, axis, normalize=False):
            if buf is None:
                return run(lambda x_: place(x_, gain_row, None, at, axis, normalize), x)
            return run(lambda x_, b: place(x_, gain_row, b, at, axis, normalize), x, buf)

        wq_all = put(w_query, None, SLOT[0], 1)
        wkv_all = put(w_kv, None, SLOT[0], 1)
        wo_all = put(w_out, None, SLOT[0], 0)
        normed = put(flat(hid_mine), None, 0, 0, True)
        grads = put(flat(g_mine), None, 0, 0)
        normed = put(flat(hid1), normed, 1, 0, True)
        wkv_all = put(wkv1, wkv_all, SLOT[1], 1)
        wq_all = put(wq1, wq_all, SLOT[1], 1)
        wo_all = put(wo1, wo_all, SLOT[1], 0)
        grads = put(flat(grd1), grads, 1, 0)
        wkv3 = send(after(wkv2), mates[1])
        wkv_all = put(wkv2, wkv_all, SLOT[2], 1)
        wkv_all = put(wkv3, wkv_all, SLOT[3], 1)
        normed = put(flat(hid2), normed, 2, 0, True)

        pos_loc, pos_rem = jnp.stack(pos_loc), jnp.stack(pos_rem)
        pos_loc, pos_rem = after((pos_loc, pos_rem))
        idx_of = lambda dev: (jnp.stack([dev ^ p for p in range(4)])[:, None] * span + jnp.arange(span)).astype(jnp.int32)
        q_idx, r_idx = idx_of(me), idx_of(2 * (chips - 1 - me // 2) + core)
        q_full = jnp.broadcast_to(q_idx[:, None, :], pos_loc.shape)
        qinfo = jnp.stack([q_full, q_full - pos_loc], axis=-1)
        qinfo = jnp.moveaxis(qinfo, 1, 0).reshape(rows, toks, 2)
        kinfo = jnp.concatenate([r_idx.reshape(1, toks), q_idx.reshape(1, toks)], axis=1)
        inv_freq = ROPE_BASE ** (-jnp.arange(0, HEAD_DIM, 2, dtype=F32) / HEAD_DIM)
        lane_freq = jnp.repeat(inv_freq, 2)
        lane_sign = jnp.where(jnp.arange(HEAD_DIM) % 2 == 0, -1.0, 1.0).astype(F32)

        def tables(pos):
            ang = pos.astype(F32)[..., None] * lane_freq
            return jnp.cos(ang), jnp.sin(ang) * lane_sign

        cos_l, sin_l = tables(pos_loc)
        cos_r, sin_r = tables(pos_rem)
        cos2, sin2 = flat(cos_l), flat(sin_l)
        cos2, sin2, qinfo, kinfo, cos_r, sin_r = lax.optimization_barrier((cos2, sin2, qinfo, kinfo, cos_r, sin_r))
        last[:] = [cos2]
        tabs = (four(cos2), four(sin2), cos_r, sin_r)

        early = [run(lambda x, w: project(x, w, cos2, sin2, 2 * i, 2, 1, (0, 3 * half)), normed, wkv_all) for i in range(2)]
        wq3 = send(after(wq2), mates[1])
        wq_all = put(wq2, wq_all, SLOT[2], 1)
        wq_all = put(wq3, wq_all, SLOT[3], 1)
        normed = put(flat(hid3), normed, 3, 0, True)

        kvs, kv_in = [], []
        for i in range(2):
            kv = four(run(lambda x, w, e: project(x, w, cos2, sin2, 2 * i, 2, 1, (3, half), e), normed, wkv_all, early[i]))
            kvs.append(kv)
            kv_in.append(send(kv, later))
        q_all = four(run(lambda x, w: project(x, w, cos2, sin2, 0, 2 * q_cols // HEAD_DIM, 2), normed, wq_all))
        wo3 = send(after(wo2), mates[1])
        wo_all = put(wo2, wo_all, SLOT[2], 0)
        wo_all = put(wo3, wo_all, SLOT[3], 0)
        head_grad = lambda g, w: dot(g, w, NT).astype(BF16).reshape(rows, span, -1)
        dos = [run(head_grad, flat(g), wo_all) for g in (g_mine, grd1, grd2)]
        grads = put(flat(grd2), grads, 2, 0)
        heads = None
        for g in GROUPS:
            local, far_in = kvs[SLOT[g] // 2], kv_in[SLOT[g ^ 2] // 2]
            if heads is None:
                heads = run(lambda q, kv, kr: attn_forward(g, q, kv, kr, qinfo, kinfo, None), q_all, local, far_in)
            else:
                if SLOT[g] == 2:
                    dos.append(run(head_grad, flat(grd3), wo_all))
                    grads = put(flat(grd3), grads, 3, 0)
                heads = run(lambda q, kv, kr, h: attn_forward(g, q, kv, kr, qinfo, kinfo, h), q_all, local, far_in, heads)
        heads_flat = flat(heads)
        att = [None] * 4
        out2, out3 = run(lambda h, w: head_out(h, w, 1, (BF16, BF16)), heads_flat, wo_all)
        att[2], att[3] = send(out2, mates[2]), send(out3, mates[3])

        dq, dkv, dkv_in = None, [None, None], [None] * 4
        for g in GROUPS:
            i = SLOT[g] // 2
            bufs = [b for b in (dq, dkv[i]) if b is not None]
            given = tuple(b is not None for b in (dq, dkv[i]))

            def fn(q, kv, kr, d0, d1, d2, d3, *rest):
                it = iter(rest)
                return attn_backward(g, q, kv, kr, (d0, d1, d2, d3), qinfo, kinfo, tabs, [next(it) if ok else None for ok in given])

            dq, dkv[i], dkr = run(fn, q_all, kvs[i], kv_in[SLOT[g ^ 2] // 2], *dos, *bufs)
            dkv_in[g ^ 2] = send(dkr, earlier)

        def add_far(mine, *theirs):
            return flat((mine + jnp.concatenate(theirs, axis=-1).astype(F32)).astype(BF16))

        cut = lambda x, s, n: x[:, s * q_cols:(s + n) * q_cols]
        low = lambda x: x.astype(BF16)
        kv_half = 2 * HEAD_DIM
        mine_half, other_half = core.astype(jnp.int32)[None], (1 - core).astype(jnp.int32)[None]
        flat_shape = (all_rows * span, width)
        hid_flat, g_flat = flat(hidden), flat(grad_out)
        dq_flat = flat(dq)
        spq13 = send(run(lambda d, n: low(dot(n, cut(d, 0, 2), TN)), dq_flat, normed), mates[1])
        dkv_a = run(add_far, dkv[0], *[dkv_in[g] for g in GROUPS[:2]])
        spk13 = send(run(lambda d, n: low(dot(n, d, TN)), dkv_a, normed), mates[1])
        spq2 = send(run(lambda d, n, e: low(dot(n, cut(d, 3, 1), TN) + e[:, q_cols:].astype(F32)), dq_flat, normed, spq13), pair)
        dkv_b = run(add_far, dkv[1], *[dkv_in[g] for g in GROUPS[2:]])
        gn = [None] * 4
        for p in (2, 3):
            gn[p] = send(run(lambda *x: grad_in(*x, p, (BF16,))[0], dq_flat, dkv_a, dkv_b, wq_all, wkv_all), mates[p])
        gn2, gn3 = gn[2], gn[3]
        spk2 = send(run(lambda d, n, e: low(dot(n, d[:, kv_half:], TN) + e[:, kv_half:].astype(F32)), dkv_b, normed, spk13), pair)
        so13 = send(run(lambda h, g: low(dot(cut(h, 0, 2), g, TN)), heads_flat, grads), mates[1])
        attn_out, out1 = run(lambda h, w, x, f: head_out_own(mine_half, h, w, x, f), heads_flat, wo_all, hid_flat, flat(att[2]))
        att[1] = send(out1, mates[1])
        own_wo, so2 = run(grad_out_rest, heads_flat, grads, so13)
        so2 = send(so2, pair)
        own_in, gn1 = run(lambda d, a, b, wq, wk: grad_in(d, a, b, wq, wk, 0, (F32, BF16)), dq_flat, dkv_a, dkv_b, wq_all, wkv_all)
        gn1 = send(gn1, mates[1])
        attn_out = run(lambda x, a, b, o: half_rows_call(residual_kernel, other_half, (x, a, b), None, o, flat_shape, False)[0], hid_flat, flat(att[1]), flat(att[3]), attn_out)
        back_call = lambda h, arrays, buf: half_rows_call(norm_back_kernel, h, arrays, gain_row, buf, flat_shape, True)
        grad_hidden, part_a = run(lambda x, g, a, b: back_call(mine_half, (x, g, a, b), None), hid_flat, g_flat, own_in, gn2)
        dwq = run(lambda d, n, e, f: dot(n, cut(d, 2, 1), TN) + (e[:, :q_cols].astype(F32) + f.astype(F32)), dq_flat, normed, spq13, spq2)
        own_kv = after(run(lambda d, n, e: dot(n, d[:, :kv_half], TN) + e[:, :kv_half].astype(F32), dkv_b, normed, spk13))
        add_cols = lambda cols: (lambda a, b: a[:, cols] + b[:, cols].astype(F32))
        dwk, dwv = run(lambda a, b: (add_cols(slice(0, HEAD_DIM))(a, b), add_cols(slice(HEAD_DIM, kv_half))(a, b)), own_kv, spk2)
        grad_hidden, part_b = run(lambda x, g, a, b, o: back_call(other_half, (x, g, a, b), o), hid_flat, g_flat, gn1, gn3, grad_hidden)
        gain_sum = jnp.sum(part_a + part_b, axis=0).reshape(-1, HEAD_DIM)
        for perm in (mates[1], mates[2], pair):
            gain_sum = gain_sum + send(gain_sum, perm)
        dwo = run(lambda a, b: a + b.astype(F32), own_wo, so2)
        return attn_out.reshape(hidden.shape), grad_hidden.reshape(hidden.shape), gain_sum.reshape(-1), dwq, dwk, dwv, dwo

    row_spec = P('dp', 'tp', None)
    tok_spec = P('dp', 'tp')
    col_spec = P(None, 'tp')
    return jax.shard_map(
        device_step, mesh=mesh,
        in_specs=(row_spec, tok_spec, tok_spec, P(), col_spec, col_spec, col_spec, P('tp', None), row_spec),
        out_specs=(row_spec, row_spec, P('dp'), P('dp', 'tp'), P('dp', 'tp'), P('dp', 'tp'), P(('dp', 'tp'), None)),
        check_vma=False)
```
